32 devices in a mesh: parts: 2 (over y), space: 4 (over z), tm: 2 (over x), spin: 2 (over core).
Axes of the slice: x: 2, y: 2, z: 4, core: 2. Of those that a mesh axis runs over, the one named last changes fastest.
Arguments:
- backward: bfloat16 [4, 2, 4, 64, 3, 4, 128], P('parts', 'tm', None, 'spin', None, 'space'), parts along dimension 0, may hold values from -6 to 6
- forward: bfloat16 [4, 2, 4, 64, 3, 4, 128], P('parts', 'tm', None, 'spin', None, 'space'), parts along dimension 0, may hold values from -6 to 6
- gauge_links: bfloat16 [4, 3, 3, 3, 2, 4, 128], P('parts', None, None, None, 'tm', 'space'), parts along dimension 0, may hold values from -2.5 to 2.5
- momenta: int32 [3, 3], replicated, may hold values from -2 to 2
- gamma_list: int32 [16], replicated, may hold values from 0 to 15
Outputs:
- insertion: float32 [4, 3, 16, 2, 64, 64], P('parts', None, None, 'tm', 'space', 'spin'), parts along dimension 0
The draws below stay inside these ranges and needn't reach their ends.
There are 2 independent parts, one for each index of `parts`. The reference program is written for one: setup_inputs(seed, part) draws one part's arguments, and reference() takes and returns one part's arrays. A program takes and returns all parts, laid end to end along the dimension named above; an argument that names none is the same for every part. Nothing has to cross between parts.
All inputs are finite; a program needn't handle non-finite values.
Results may differ from the reference program's by a relative error of at most 0.0056.
Values may be sent and summed in bfloat16 or wider, within the bound.
A program may use at most 64 MiB of HBM per device.

```python
import math
import jax
import jax.numpy as jnp
import numpy as np
from jax import lax

LX = 32
LY = 4
NCOL = 64
NGAM = 16
NMOM = 3
LZ = 4
SLAB = 2


def with_ends(values, rng, low, top_value):
    index_at = [jax.random.randint(jax.random.fold_in(rng, axis), (), 0, length) for axis, length in enumerate(values.shape)]
    widest = values.shape.index(max(values.shape))
    neighbour = index_at[:widest] + [(index_at[widest] + 1) % values.shape[widest]] + index_at[widest + 1:]
    return values.at[tuple(index_at)].set(low).at[tuple(neighbour)].set(top_value)


def block_scale(stream_key, extent, cuts, low, high):
    factor_of = 1.0
    for axis_at, parts in cuts:
        draws = jax.random.uniform(jax.random.fold_in(jax.random.fold_in(stream_key, 6), axis_at), (parts,), jnp.float32, low / len(cuts), high / len(cuts))
        factor_of = factor_of * jnp.repeat(jnp.exp(draws), extent[axis_at] // parts).reshape((-1,) + (1,) * (len(extent) - 1 - axis_at))
    return factor_of


def bell_draw(rng, extent, width, reach, split=(), kind=jnp.bfloat16):
    entries = width * jax.random.normal(rng, extent, jnp.float32)
    if split:
        entries = entries * block_scale(rng, extent, split, -0.22, 0.18)
    return jnp.clip(entries, -reach, reach).astype(kind)


def setup_inputs(seed: int = 0, part: int = 0) -> dict:
    splits = jax.random.split(jax.random.key(seed), 6)
    own_keys = jax.random.split(jax.random.fold_in(splits[5], part), 6)
    return {
        "backward": bell_draw(own_keys[0], (2, SLAB, 4, NCOL, 3, LZ, LX * LY), 1.0, 6.0, ((1, 2), (3, 2), (5, 4))),
        "forward": bell_draw(own_keys[1], (2, SLAB, 4, NCOL, 3, LZ, LX * LY), 1.0, 6.0, ((1, 2), (3, 2), (5, 4))),
        "gauge_links": bell_draw(own_keys[2], (2, 3, 3, 3, SLAB, LZ, LX * LY), 0.41, 2.5, ((4, 2), (5, 4))),
        "momenta": with_ends(jax.random.randint(splits[3], (NMOM, 3), -2, 3), jax.random.fold_in(splits[3], 1), -2, 2).astype(jnp.int32),
        "gamma_list": with_ends(jax.random.randint(splits[4], (NGAM,), 0, 16), jax.random.fold_in(splits[4], 1), 0, 15).astype(jnp.int32),
    }


def gamma_tables():
    zeros = np.zeros((4, 4))
    gx_imag = np.array([[0, 0, 0, 1], [0, 0, 1, 0], [0, -1, 0, 0], [-1, 0, 0, 0]]) * 1.0
    gy_real = np.array([[0, 0, 0, -1], [0, 0, 1, 0], [0, 1, 0, 0], [-1, 0, 0, 0]]) * 1.0
    gz_imag = np.array([[0, 0, 1, 0], [0, 0, 0, -1], [-1, 0, 0, 0], [0, 1, 0, 0]]) * 1.0
    gt_real = np.array([[0, 0, 1, 0], [0, 0, 0, 1], [1, 0, 0, 0], [0, 1, 0, 0]]) * 1.0
    singles = [(zeros, gx_imag), (gy_real, zeros), (zeros, gz_imag), (gt_real, zeros)]
    clif_real = []
    clif_imag = []
    for number in range(16):
        mat_real = np.eye(4)
        mat_imag = np.zeros((4, 4))
        for which in range(4):
            if number >> which & 1:
                other_real, other_imag = singles[which]
                new_real = mat_real @ other_real - mat_imag @ other_imag
                new_imag = mat_real @ other_imag + mat_imag @ other_real
                mat_real, mat_imag = (new_real, new_imag)
        clif_real.append(mat_real)
        clif_imag.append(mat_imag)
    return (singles, (np.stack(clif_real), np.stack(clif_imag)))

def chosen_gammas(gamma_list):
    singles, clifford = gamma_tables()
    table_real = jnp.asarray(clifford[0], dtype=jnp.float32)
    table_imag = jnp.asarray(clifford[1], dtype=jnp.float32)
    one_hot = (gamma_list[:, None] == jnp.arange(16, dtype=jnp.int32)[None, :]).astype(jnp.float32)
    gam_real = jnp.einsum('kg,gsv->ksv', one_hot, table_real, precision=lax.Precision.HIGHEST)
    gam_imag = jnp.einsum('kg,gsv->ksv', one_hot, table_imag, precision=lax.Precision.HIGHEST)
    return (gam_real, gam_imag)

def color_apply(link_real, link_imag, spin_real, spin_imag, dagger):
    outs_real = []
    outs_imag = []
    for c in range(3):
        summed_real = 0.0
        summed_imag = 0.0
        for d in range(3):
            if dagger:
                coef_real = link_real[d, c]
                coef_imag = -link_imag[d, c]
            else:
                coef_real = link_real[c, d]
                coef_imag = link_imag[c, d]
            coef_real = coef_real[..., None, None, :, :]
            coef_imag = coef_imag[..., None, None, :, :]
            part_real = spin_real[..., d, :, :]
            part_imag = spin_imag[..., d, :, :]
            summed_real = summed_real + coef_real * part_real - coef_imag * part_imag
            summed_imag = summed_imag + coef_real * part_imag + coef_imag * part_real
        outs_real.append(summed_real)
        outs_imag.append(summed_imag)
    return (jnp.stack(outs_real, axis=-3), jnp.stack(outs_imag, axis=-3))

def spin_apply(matrix, spin_real, spin_imag):
    outs_real = []
    outs_imag = []
    for t in range(4):
        summed_real = 0.0
        summed_imag = 0.0
        for s in range(4):
            coef_real = float(matrix[0][t, s])
            coef_imag = float(matrix[1][t, s])
            if coef_real == 0.0 and coef_imag == 0.0:
                continue
            part_real = spin_real[..., s, :, :, :, :]
            part_imag = spin_imag[..., s, :, :, :, :]
            summed_real = summed_real + coef_real * part_real - coef_imag * part_imag
            summed_imag = summed_imag + coef_real * part_imag + coef_imag * part_real
        outs_real.append(summed_real)
        outs_imag.append(summed_imag)
    return (jnp.stack(outs_real, axis=-5), jnp.stack(outs_imag, axis=-5))

def plane_roll(spinor, offset, along_y, width_x):
    initial = spinor.shape
    gridded = spinor.reshape(initial[:-1] + (initial[-1] // width_x, width_x))
    gridded = jnp.roll(gridded, offset, axis=-2 if along_y else -1)
    return gridded.reshape(initial)

def current(fwd_real, fwd_imag, link_real, link_imag, up_z, down_z, width_x):
    singles, clifford = gamma_tables()
    summed_real = 0.0
    summed_imag = 0.0
    for direction in range(3):
        single_real, single_imag = singles[direction]
        minus_proj = ((np.eye(4) - single_real) / 2.0, -single_imag / 2.0)
        plus_proj = ((np.eye(4) + single_real) / 2.0, single_imag / 2.0)
        if direction < 2:
            along_y = direction == 1
            up_real = plane_roll(fwd_real, -1, along_y, width_x)
            up_imag = plane_roll(fwd_imag, -1, along_y, width_x)
            back_real, back_imag = color_apply(link_real[direction], link_imag[direction], fwd_real, fwd_imag, True)
            down_real = plane_roll(back_real, 1, along_y, width_x)
            down_imag = plane_roll(back_imag, 1, along_y, width_x)
        else:
            up_real, up_imag = up_z
            down_real, down_imag = down_z
        hop_real, hop_imag = color_apply(link_real[direction], link_imag[direction], up_real, up_imag, False)
        ahead_real, ahead_imag = spin_apply(minus_proj, hop_real, hop_imag)
        behind_real, behind_imag = spin_apply(plus_proj, down_real, down_imag)
        summed_real = summed_real + ahead_real - behind_real
        summed_imag = summed_imag + ahead_imag - behind_imag
    return (summed_real, summed_imag)

def phase_list(momenta, z_start, layers, plane_size, width_x, width_y, full_z):
    sites = jnp.arange(plane_size, dtype=jnp.int32)
    coord_x = sites % width_x
    coord_y = sites // width_x
    coord_z = z_start + jnp.arange(layers, dtype=jnp.int32)
    result = []
    for number in range(momenta.shape[0]):
        frac_plane = jnp.mod(momenta[number, 0] * coord_x, width_x).astype(jnp.float32) / float(width_x)
        frac_plane = frac_plane + jnp.mod(momenta[number, 1] * coord_y, width_y).astype(jnp.float32) / float(width_y)
        frac_depth = jnp.mod(momenta[number, 2] * coord_z, full_z).astype(jnp.float32) / float(full_z)
        result.append(2.0 * math.pi * (frac_depth[:, None] + frac_plane[None, :]))
    return result

def contract(back_piece, weave_re, weave_im, thetas, gam_real, gam_imag, scaling):
    back_real = back_piece[0].astype(jnp.float32)
    back_imag = back_piece[1].astype(jnp.float32)
    slab_times, spins, columns = (back_real.shape[0], back_real.shape[1], back_real.shape[2])
    blocks = []
    for theta in thetas:
        cosine = jnp.cos(theta)
        sine_part = jnp.sin(theta)
        rot_real = lax.optimization_barrier((cosine * back_real - sine_part * back_imag).astype(jnp.bfloat16)).astype(jnp.float32)
        rot_imag = lax.optimization_barrier((sine_part * back_real + cosine * back_imag).astype(jnp.bfloat16)).astype(jnp.float32)
        stacked = jnp.concatenate([rot_real.reshape(slab_times, spins, columns, -1), rot_imag.reshape(slab_times, spins, columns, -1)], axis=-1)
        pair_real = jnp.einsum('usak,uvbk->usvab', stacked, weave_re)
        pair_imag = jnp.einsum('usak,uvbk->usvab', stacked, weave_im)
        out_real = jnp.einsum('ksv,usvab->kuab', gam_real, pair_real, precision=lax.Precision.HIGHEST) - jnp.einsum('ksv,usvab->kuab', gam_imag, pair_imag, precision=lax.Precision.HIGHEST)
        out_imag = jnp.einsum('ksv,usvab->kuab', gam_real, pair_imag, precision=lax.Precision.HIGHEST) + jnp.einsum('ksv,usvab->kuab', gam_imag, pair_real, precision=lax.Precision.HIGHEST)
        blocks.append(jnp.stack([out_real, out_imag]) * scaling)
    return jnp.stack(blocks, axis=1)

def reference(backward, forward, gauge_links, momenta, gamma_list):
    layers = forward.shape[5]
    plane_size = forward.shape[6]
    width_x = LX
    thetas = phase_list(momenta, jnp.int32(0), layers, plane_size, width_x, plane_size // width_x, layers)
    gam_real, gam_imag = chosen_gammas(gamma_list)
    scaling = 1.0 / math.sqrt(3.0 * plane_size * layers)

    def one_time(slices):
        back_slice, fwd_slice, link_slice = slices
        fwd_real = fwd_slice[0][None].astype(jnp.float32)
        fwd_imag = fwd_slice[1][None].astype(jnp.float32)
        link_real = link_slice[0][:, :, :, None].astype(jnp.float32)
        link_imag = link_slice[1][:, :, :, None].astype(jnp.float32)
        up_z = (jnp.roll(fwd_real, -1, axis=-2), jnp.roll(fwd_imag, -1, axis=-2))
        back_real, back_imag = color_apply(link_real[2], link_imag[2], fwd_real, fwd_imag, True)
        down_z = (jnp.roll(back_real, 1, axis=-2), jnp.roll(back_imag, 1, axis=-2))
        weave_real, weave_imag = current(fwd_real, fwd_imag, link_real, link_imag, up_z, down_z, width_x)
        woven_real = lax.optimization_barrier(weave_real.astype(jnp.bfloat16)).astype(jnp.float32)
        woven_imag = lax.optimization_barrier(weave_imag.astype(jnp.bfloat16)).astype(jnp.float32)
        flat_real = woven_real.reshape(woven_real.shape[0], 4, woven_real.shape[2], -1)
        flat_imag = woven_imag.reshape(woven_imag.shape[0], 4, woven_imag.shape[2], -1)
        weave_re = jnp.concatenate([flat_real, flat_imag], axis=-1)
        weave_im = jnp.concatenate([flat_imag, -flat_real], axis=-1)
        result = contract(back_slice[:, None], weave_re, weave_im, thetas, gam_real, gam_imag, scaling)
        return result[:, :, :, 0]
    stacked = lax.map(one_time, (jnp.moveaxis(backward, 1, 0), jnp.moveaxis(forward, 1, 0), jnp.moveaxis(gauge_links, 4, 0)))
    return jnp.moveaxis(stacked, 0, 3)
```

```python
import functools
import math

import jax
import jax.numpy as jnp
import numpy as np
from jax import lax
from jax.experimental import pallas as pl
from jax.experimental.pallas import tpu as pltpu
from jax.sharding import PartitionSpec as P

LX = 32
GROUP = 16
LINE = 4


def gamma_tables():
    zeros = np.zeros((4, 4))
    gx_imag = np.array([[0, 0, 0, 1], [0, 0, 1, 0], [0, -1, 0, 0], [-1, 0, 0, 0]]) * 1.0
    gy_real = np.array([[0, 0, 0, -1], [0, 0, 1, 0], [0, 1, 0, 0], [-1, 0, 0, 0]]) * 1.0
    gz_imag = np.array([[0, 0, 1, 0], [0, 0, 0, -1], [-1, 0, 0, 0], [0, 1, 0, 0]]) * 1.0
    gt_real = np.array([[0, 0, 1, 0], [0, 0, 0, 1], [1, 0, 0, 0], [0, 1, 0, 0]]) * 1.0
    singles = [zeros + 1j * gx_imag, gy_real + 0j, 1j * gz_imag, gt_real + 0j]
    basis = []
    for number in range(16):
        matrix = np.eye(4) + 0j
        for which in range(4):
            if number >> which & 1:
                matrix = matrix @ singles[which]
        basis.append(matrix)
    return singles, np.stack(basis)


def unit_times(unit, value):
    real, imag = value
    if unit == 1:
        return real, imag
    if unit == -1:
        return -real, -imag
    if unit == 1j:
        return -imag, real
    return imag, -real


def small_times(matrix, half):
    outs = []
    for row in range(2):
        column = int(np.flatnonzero(matrix[row])[0])
        outs.append([unit_times(complex(matrix[row, column]), value) for value in half[column]])
    return outs


def added(first, second):
    return [
        [(a[0] + b[0], a[1] + b[1]) for a, b in zip(left, right)]
        for left, right in zip(first, second)
    ]


def subtracted(first, second):
    return [
        [(a[0] - b[0], a[1] - b[1]) for a, b in zip(left, right)]
        for left, right in zip(first, second)
    ]


def kernel(
    spaces,
    width_x,
    full_z,
    back_hbm,
    fwd_hbm,
    link_hbm,
    momenta_ref,
    gamma_ref,
    table_hbm,
    out_ref,
    back_ref,
    fwd_ref,
    link_ref,
    table_ref,
    other_back,
    chosen_ref,
    links,
    halo_send,
    halo_recv,
    rows_scr,
    weave,
    weave_mm,
    pair,
    chunk_send,
    chunk_recv,
    load_sems,
    back_sems,
    halo_send_sems,
    halo_recv_sems,
    chunk_send_sems,
    chunk_recv_sems,
    ready_sem,
):
    loads = [
        pltpu.make_async_copy(source, target, load_sems.at[number])
        for number, (source, target) in enumerate(
            (
                (fwd_hbm, fwd_ref),
                (link_hbm, link_ref),
                (back_hbm, back_ref),
                (table_hbm, table_ref),
            )
        )
    ]
    for load in loads:
        load.start()
    columns = fwd_ref.shape[3]
    plane = fwd_ref.shape[4]
    moments = momenta_ref.shape[0]
    gammas = gamma_ref.shape[0]
    groups = columns // GROUP
    rows = columns * 2 // spaces
    last = spaces - 1
    relayed = 4 <= spaces <= LINE
    here = lax.axis_index("space")
    core = lax.axis_index("spin")
    after = lax.rem(here + 1, spaces)
    before = lax.rem(here + last, spaces)
    singles, _ = gamma_tables()

    barrier = pltpu.get_barrier_semaphore()
    for step in range(1, spaces):
        pl.semaphore_signal(
            barrier, inc=1, device_id={"space": lax.rem(here + step, spaces)}
        )

    @pl.when(core == 0)
    def _():
        pl.semaphore_signal(barrier, inc=1, device_id={"spin": 1 - core})

    if relayed:
        for g in range(groups):
            for number in range(moments):

                @pl.when(here == 0)
                def _(g=g, number=number):
                    chunk_recv[g, number, 0] = jnp.zeros_like(chunk_recv[g, number, 0])

                @pl.when(here == last)
                def _(g=g, number=number):
                    chunk_recv[g, number, last - 1] = jnp.zeros_like(chunk_recv[g, number, 0])

    for load in loads[:2]:
        load.wait()
    for mu in range(3):
        for c in range(3):
            for d in range(3):
                row = ((mu * 3 + c) * 3 + d) * 2
                links[row : row + 2, :] = link_ref[mu, c, d].astype(jnp.float32)

    def link(mu, c, d):
        row = ((mu * 3 + c) * 3 + d) * 2
        return [
            jnp.broadcast_to(links[row + part : row + part + 1, :], (GROUP, plane))
            for part in range(2)
        ]

    def colour(mu, half, dagger):
        outs = [[None] * 3 for _ in range(2)]
        for c in range(3):
            for d in range(3):
                u_real, u_imag = link(mu, d, c) if dagger else link(mu, c, d)
                for spin in range(2):
                    v_real, v_imag = half[spin][d]
                    if dagger:
                        real = u_real * v_real + u_imag * v_imag
                        imag = u_real * v_imag - u_imag * v_real
                    else:
                        real = u_real * v_real - u_imag * v_imag
                        imag = u_real * v_imag + u_imag * v_real
                    held = outs[spin][c]
                    outs[spin][c] = (
                        (real, imag) if held is None else (held[0] + real, held[1] + imag)
                    )
        return outs

    lanes = lax.broadcasted_iota(jnp.int32, (GROUP, plane), 1)
    column_x = lax.rem(lanes, width_x)

    def rolled(value, steps, along_y):
        if along_y:
            return pltpu.roll(value, (steps * width_x) % plane, 1)
        plain = pltpu.roll(value, steps % plane, 1)
        wrapped = pltpu.roll(value, (steps - steps * width_x) % plane, 1)
        edge = 0 if steps == 1 else width_x - 1
        return jnp.where(column_x == edge, wrapped, plain)

    def rolled_half(half, steps, along_y):
        return [
            [tuple(rolled(part, steps, along_y) for part in value) for value in spin]
            for spin in half
        ]

    def spinor(cols):
        return [
            [
                tuple(fwd_ref[part, s, c, cols, :].astype(jnp.float32) for part in range(2))
                for c in range(3)
            ]
            for s in range(4)
        ]

    def group(index):
        if isinstance(index, int):
            return slice(index * GROUP, (index + 1) * GROUP)
        return pl.ds(pl.multiple_of(index * GROUP, GROUP), GROUP)

    def halo_copy(g, side):
        return pltpu.make_async_remote_copy(
            src_ref=halo_send.at[g, side],
            dst_ref=halo_recv.at[g, side],
            send_sem=halo_send_sems.at[g, side],
            recv_sem=halo_recv_sems.at[g, side],
            device_id={"space": before if side == 0 else after},
        )

    for g in range(groups):
        psi = spinor(group(g))
        turned = small_times(singles[2][:2, 2:], psi[2:])
        minus = subtracted(psi[:2], turned)
        plus = colour(2, added(psi[:2], turned), True)
        for side, half in enumerate((minus, plus)):
            for spin in range(2):
                for c in range(3):
                    for part in range(2):
                        halo_send[g, side, part, spin, c] = half[spin][c][part].astype(
                            jnp.bfloat16
                        )
        if g == 0:
            pl.semaphore_wait(barrier, last + core)

        @pl.when(here == last)
        def _(g=g):
            halo_copy(g, 1).start()
            halo_copy(g, 0).start()

        @pl.when(here != last)
        def _(g=g):
            halo_copy(g, 0).start()
            halo_copy(g, 1).start()

    loads[2].wait()
    back_copy = pltpu.make_async_remote_copy(
        src_ref=back_ref,
        dst_ref=other_back,
        send_sem=back_sems.at[0],
        recv_sem=back_sems.at[1],
        device_id={"spin": 1 - core},
    )

    @pl.when(core == 1)
    def _():
        pl.semaphore_signal(ready_sem, inc=1, device_id={"spin": 1 - core})
        back_copy.start()

    def store_weave(cols, full, first):
        for s in range(4):
            for c in range(3):
                for part in range(2):
                    value = full[s][c][part]
                    if not first:
                        value = value + weave[part, s, c, cols, :]
                    weave[part, s, c, cols, :] = value

    def plane_group(index, carry):
        cols = group(index)
        psi = spinor(cols)
        upper = lower = None
        for mu in range(2):
            turned = small_times(singles[mu][:2, 2:], psi[2:])
            ahead = colour(mu, rolled_half(subtracted(psi[:2], turned), -1, mu == 1), False)
            behind = rolled_half(colour(mu, added(psi[:2], turned), True), 1, mu == 1)
            up = subtracted(ahead, behind)
            low = small_times(-singles[mu][2:, :2], added(ahead, behind))
            upper = up if upper is None else added(upper, up)
            lower = low if lower is None else added(lower, low)
        store_weave(cols, upper + lower, True)
        return carry

    lax.fori_loop(0, groups, plane_group, 0)

    sites = lax.broadcasted_iota(jnp.int32, (8, plane), 1)
    coord_x = lax.rem(sites, width_x).astype(jnp.float32)
    coord_y = lax.div(sites, width_x).astype(jnp.float32)
    coord_z = here.astype(jnp.float32)
    phases = []
    for number in range(moments):
        momentum = [momenta_ref[number, axis].astype(jnp.float32) for axis in range(3)]
        turns = coord_x * (momentum[0] * (1.0 / width_x))
        turns = turns + coord_y * (momentum[1] * (width_x / plane))
        turns = turns + coord_z * (momentum[2] * (1.0 / full_z))
        theta = (2.0 * math.pi) * (turns - jnp.floor(turns))
        phases.append((jnp.cos(theta)[:1, :], jnp.sin(theta)[:1, :]))

    loads[3].wait()
    for k in range(gammas):
        chosen_ref[k] = table_ref[gamma_ref[k]]

    def arrange(owner, source):
        for part in range(2):
            for c in range(3):
                lane = (part * 3 + c) * plane
                for s in range(4):
                    for j in range(columns // rows):
                        row = (j * 4 + s) * rows
                        rows_scr[owner, row : row + rows, lane : lane + plane] = source[
                            part, s, c, j * rows : (j + 1) * rows, :
                        ]

    arrange(core, back_ref)

    @pl.when(core == 0)
    def _():
        pl.semaphore_wait(ready_sem, 1)
        back_copy.start()

    back_copy.wait_recv()
    arrange(1 - core, other_back)

    def is_long(step):
        if not relayed or step not in (1, last):
            return None
        return here == (last if step == 1 else 0)

    inner = (here != 0) & (here != last)
    far = jnp.where(here == 1, last, 0)

    def chunk_copy(g, number, step):
        target = source = lax.rem(here + step, spaces)
        slot = step - 1
        long = is_long(step)
        if long is not None:
            target = jnp.where(long, last - 1 if step == 1 else 1, target)
            slot = jnp.where(long, last, slot)
        return pltpu.make_async_remote_copy(
            src_ref=chunk_send.at[g, number, source],
            dst_ref=chunk_recv.at[g, number, slot],
            send_sem=chunk_send_sems.at[g, number, step - 1],
            recv_sem=chunk_recv_sems.at[g, number, slot],
            device_id={"space": target},
        )

    def wait_chunk(g, number, slot):
        pltpu.make_async_remote_copy(
            src_ref=chunk_send.at[g, number, 0],
            dst_ref=chunk_recv.at[g, number, slot],
            send_sem=chunk_send_sems.at[g, number, 0],
            recv_sem=chunk_recv_sems.at[g, number, slot],
            device_id={"space": after},
        ).wait_recv()

    chunk_rows = 4 * rows
    order = sorted(range(1, spaces), key=lambda step: -min(step, spaces - step))
    if relayed:
        order = [last, 1] + [step for step in order if step not in (1, last)]
    for g in range(groups):
        for side in range(2):
            halo_copy(g, side).wait_recv()
        received = [
            [
                [
                    tuple(
                        halo_recv[g, side, part, spin, c].astype(jnp.float32)
                        for part in range(2)
                    )
                    for c in range(3)
                ]
                for spin in range(2)
            ]
            for side in range(2)
        ]
        ahead = colour(2, received[0], False)
        behind = received[1]
        upper = subtracted(ahead, behind)
        lower = small_times(-singles[2][2:, :2], added(ahead, behind))
        cols = group(g)
        store_weave(cols, upper + lower, False)
        for number in range(moments):
            cosine, sine = phases[number]
            for s in range(4):
                for c in range(3):
                    real = weave[0, s, c, cols, :]
                    imag = weave[1, s, c, cols, :]
                    turned_real = (cosine * real + sine * imag).astype(jnp.bfloat16)
                    turned_imag = (cosine * imag - sine * real).astype(jnp.bfloat16)
                    rows_at = slice(s * GROUP, (s + 1) * GROUP)
                    rows_next = slice((4 + s) * GROUP, (5 + s) * GROUP)
                    lanes_at = slice(c * plane, (c + 1) * plane)
                    lanes_next = slice((3 + c) * plane, (4 + c) * plane)
                    weave_mm[g, number, rows_at, lanes_at] = turned_real
                    weave_mm[g, number, rows_at, lanes_next] = turned_imag
                    weave_mm[g, number, rows_next, lanes_at] = turned_imag
                    weave_mm[g, number, rows_next, lanes_next] = -turned_real
            product = lax.dot_general(
                rows_scr[...].reshape(8 * columns, 6 * plane),
                weave_mm[g, number],
                (((1,), (1,)), ((), ())),
                preferred_element_type=jnp.float32,
            )
            for target in range(spaces):
                piece = product[target * chunk_rows : (target + 1) * chunk_rows]
                pair[g, number, target] = piece
                chunk_send[g, number, target] = piece.astype(jnp.bfloat16)
            for step in order:
                copy = chunk_copy(g, number, step)
                if relayed and 1 < step < last:
                    delayed = inner & (lax.rem(here + step, spaces) == far)
                    pl.when(jnp.logical_not(delayed))(copy.start)
                else:
                    copy.start()

    if relayed:
        for g in range(groups):
            for number in range(moments):
                for step in range(2, last):

                    @pl.when(((here == 1) & (step == last - 1)) | ((here == last - 1) & (step == 2)))
                    def _(g=g, number=number, step=step):
                        wait_chunk(g, number, last)
                        target = lax.rem(here + step, spaces)
                        summed = pair[g, number, target] + chunk_recv[g, number, last].astype(
                            jnp.float32
                        )
                        chunk_send[g, number, target] = summed.astype(jnp.bfloat16)
                        chunk_copy(g, number, step).start()

    width = pair.shape[-1]
    half = width // 2
    for g in range(groups):
        for number in range(moments):
            total = pair[g, number, here]
            for step in range(1, spaces):
                if relayed and step in (1, last):
                    end = 0 if step == 1 else last
                    pl.when(here != end)(
                        functools.partial(wait_chunk, g, number, step - 1)
                    )
                else:
                    wait_chunk(g, number, step - 1)
                total = total + chunk_recv[g, number, step - 1].astype(jnp.float32)
            values = [total[s * rows : (s + 1) * rows] for s in range(4)]
            turned = [pltpu.roll(value, half, 1) for value in values]
            for k in range(gammas):
                summed = None
                for s in range(4):
                    term = chosen_ref[k, s : s + 1, :] * values[s]
                    term = term + chosen_ref[k, 4 + s : 5 + s, :] * turned[s]
                    summed = term if summed is None else summed + term
                summed = summed + pltpu.roll(summed, width - GROUP, 1)
                summed = summed + pltpu.roll(summed, width - 2 * GROUP, 1)
                for part in range(2):
                    out_ref[part, number, k, :, g * GROUP : (g + 1) * GROUP] = summed[
                        :, part * half : part * half + GROUP
                    ]

    back_copy.wait_send()
    for g in range(groups):
        for side in range(2):
            halo_copy(g, side).wait_send()
        for number in range(moments):
            for step in range(1, spaces):
                chunk_copy(g, number, step).wait_send()


def store_kernel(value_ref, out_hbm, sems):
    moments = value_ref.shape[1]
    stores = [
        pltpu.make_async_copy(
            value_ref.at[:, number], out_hbm.at[:, number], sems.at[number]
        )
        for number in range(moments)
    ]
    for store in stores:
        store.start()
    for store in stores:
        store.wait()


def body(mesh, backward, forward, gauge_links, momenta, gamma_list):
    spaces = mesh.shape["space"]
    _, times, _, columns, _, layers, plane = forward.shape
    moments = momenta.shape[0]
    gammas = gamma_list.shape[0]
    rows = columns * mesh.shape["spin"] // spaces
    groups = columns // GROUP
    back = jnp.transpose(backward, (0, 1, 2, 4, 5, 3, 6)).reshape(2, 4, 3, columns, plane)
    fwd = jnp.transpose(forward, (0, 1, 2, 4, 5, 3, 6)).reshape(2, 4, 3, columns, plane)
    link = jnp.transpose(gauge_links, (1, 2, 3, 4, 5, 0, 6)).reshape(3, 3, 3, 2, plane)
    full_z = layers * spaces
    scaling = 0.5 / math.sqrt(3.0 * plane * full_z)
    _, basis = gamma_tables()
    plain = np.concatenate([basis.real, basis.real], axis=2)
    crossed = np.concatenate([-basis.imag, basis.imag], axis=2)
    table = np.concatenate([plain, crossed], axis=1)
    table = (np.repeat(table, GROUP, axis=2) * scaling).astype(np.float32)
    width = table.shape[2]
    slots = spaces if 4 <= spaces <= LINE else spaces - 1
    vmem = pl.BlockSpec(memory_space=pltpu.VMEM)
    anywhere = pl.BlockSpec(memory_space=pl.ANY)
    smem = pl.BlockSpec(memory_space=pltpu.SMEM)
    out_shape = (2, moments, gammas, rows, columns)
    values = pl.pallas_call(
        functools.partial(kernel, spaces, LX, full_z),
        out_shape=pltpu.VMEM(out_shape, jnp.float32),
        in_specs=[anywhere, anywhere, anywhere, smem, smem, anywhere],
        out_specs=vmem,
        scratch_shapes=[
            pltpu.VMEM(back.shape, back.dtype),
            pltpu.VMEM(fwd.shape, fwd.dtype),
            pltpu.VMEM(link.shape, link.dtype),
            pltpu.VMEM(table.shape, jnp.float32),
            pltpu.VMEM((2, 4, 3, columns, plane), jnp.bfloat16),
            pltpu.VMEM((gammas,) + table.shape[1:], jnp.float32),
            pltpu.VMEM((56, plane), jnp.float32),
            pltpu.VMEM((groups, 2, 2, 2, 3, GROUP, plane), jnp.bfloat16),
            pltpu.VMEM((groups, 2, 2, 2, 3, GROUP, plane), jnp.bfloat16),
            pltpu.VMEM((2, 4 * columns, 6 * plane), jnp.bfloat16),
            pltpu.VMEM((2, 4, 3, columns, plane), jnp.float32),
            pltpu.VMEM((groups, moments, width, 6 * plane), jnp.bfloat16),
            pltpu.VMEM((groups, moments, spaces, 4 * rows, width), jnp.float32),
            pltpu.VMEM((groups, moments, spaces, 4 * rows, width), jnp.bfloat16),
            pltpu.VMEM((groups, moments, slots, 4 * rows, width), jnp.bfloat16),
            pltpu.SemaphoreType.DMA((4,)),
            pltpu.SemaphoreType.DMA((2,)),
            pltpu.SemaphoreType.DMA((groups, 2)),
            pltpu.SemaphoreType.DMA((groups, 2)),
            pltpu.SemaphoreType.DMA((groups, moments, spaces - 1)),
            pltpu.SemaphoreType.DMA((groups, moments, slots)),
            pltpu.SemaphoreType.REGULAR,
        ],
        compiler_params=pltpu.CompilerParams(collective_id=0, has_side_effects=True),
    )(back, fwd, link, momenta, gamma_list, table)
    out = pl.pallas_call(
        store_kernel,
        out_shape=jax.ShapeDtypeStruct(out_shape, jnp.float32),
        in_specs=[vmem],
        out_specs=anywhere,
        scratch_shapes=[pltpu.SemaphoreType.DMA((moments,))],
    )(pltpu.with_memory_space_constraint(values, pltpu.VMEM))
    return out.reshape(2, moments, gammas, times, rows, columns)


def solution(mesh):
    in_specs = (
        P("parts", "tm", None, "spin", None, "space", None),
        P("parts", "tm", None, "spin", None, "space", None),
        P("parts", None, None, None, "tm", "space", None),
        P(),
        P(),
    )
    out_specs = P("parts", None, None, "tm", "space", "spin")
    return jax.shard_map(
        functools.partial(body, mesh),
        mesh=mesh,
        in_specs=in_specs,
        out_specs=out_specs,
        check_vma=False,
    )
```

```python
import functools
import math

import jax
import jax.numpy as jnp
import numpy as np
from jax import lax
from jax.experimental import pallas as pl
from jax.experimental.pallas import tpu as pltpu
from jax.sharding import PartitionSpec as P

LX = 32
GROUP = 16
LINE = 4


def gamma_tables():
    zeros = np.zeros((4, 4))
    gx_imag = np.array([[0, 0, 0, 1], [0, 0, 1, 0], [0, -1, 0, 0], [-1, 0, 0, 0]]) * 1.0
    gy_real = np.array([[0, 0, 0, -1], [0, 0, 1, 0], [0, 1, 0, 0], [-1, 0, 0, 0]]) * 1.0
    gz_imag = np.array([[0, 0, 1, 0], [0, 0, 0, -1], [-1, 0, 0, 0], [0, 1, 0, 0]]) * 1.0
    gt_real = np.array([[0, 0, 1, 0], [0, 0, 0, 1], [1, 0, 0, 0], [0, 1, 0, 0]]) * 1.0
    singles = [zeros + 1j * gx_imag, gy_real + 0j, 1j * gz_imag, gt_real + 0j]
    basis = []
    for number in range(16):
        matrix = np.eye(4) + 0j
        for which in range(4):
            if number >> which & 1:
                matrix = matrix @ singles[which]
        basis.append(matrix)
    return singles, np.stack(basis)


def pick_table(basis):
    table = np.zeros((len(basis), 8), np.int32)
    real = {1: 0, -1: 1, 1j: 3, -1j: 2}
    imag = {1: 2, -1: 3, 1j: 0, -1j: 1}
    for number, matrix in enumerate(basis):
        for s in range(4):
            (t,) = np.flatnonzero(matrix[s])
            unit = complex(matrix[s, t])
            table[number, s] = (real[unit] * 4 + s) * 4 + t
            table[number, 4 + s] = (imag[unit] * 4 + s) * 4 + t
    return table


def unit_times(unit, value):
    real, imag = value
    if unit == 1:
        return real, imag
    if unit == -1:
        return -real, -imag
    if unit == 1j:
        return -imag, real
    return imag, -real


def small_times(matrix, half):
    outs = []
    for row in range(2):
        column = int(np.flatnonzero(matrix[row])[0])
        outs.append([unit_times(complex(matrix[row, column]), value) for value in half[column]])
    return outs


def added(first, second):
    return [
        [(a[0] + b[0], a[1] + b[1]) for a, b in zip(left, right)]
        for left, right in zip(first, second)
    ]


def subtracted(first, second):
    return [
        [(a[0] - b[0], a[1] - b[1]) for a, b in zip(left, right)]
        for left, right in zip(first, second)
    ]


def kernel(
    spaces,
    width_x,
    full_z,
    scaling,
    back_hbm,
    fwd_hbm,
    link_hbm,
    momenta_hbm,
    gamma_hbm,
    table_hbm,
    out_ref,
    back_ref,
    fwd_ref,
    link_ref,
    table_ref,
    momenta_ref,
    gamma_ref,
    other_back,
    folded,
    links,
    halo_send,
    halo_recv,
    rows_scr,
    weave,
    weave_mm,
    pair,
    chunk_send,
    chunk_recv,
    relay_recv,
    load_sems,
    back_sems,
    halo_send_sem,
    halo_recv_sems,
    chunk_send_sem,
    chunk_recv_sems,
    relay_sems,
    ready_sem,
):
    loads = [
        pltpu.make_async_copy(source, target, load_sems.at[number])
        for number, (source, target) in enumerate(
            (
                (fwd_hbm, fwd_ref),
                (link_hbm, link_ref),
                (back_hbm, back_ref),
                (table_hbm, table_ref),
                (momenta_hbm, momenta_ref),
                (gamma_hbm, gamma_ref),
            )
        )
    ]
    for load in loads:
        load.start()
    columns = fwd_ref.shape[3]
    plane = fwd_ref.shape[4]
    moments = momenta_ref.shape[0]
    gammas = gamma_ref.shape[0]
    groups = columns // GROUP
    rows = columns * 2 // spaces
    last = spaces - 1
    relayed = 4 <= spaces <= LINE
    here = lax.axis_index("space")
    core = lax.axis_index("spin")
    after = lax.rem(here + 1, spaces)
    before = lax.rem(here + last, spaces)
    singles, _ = gamma_tables()

    barrier = pltpu.get_barrier_semaphore()
    for step in range(1, spaces):
        pl.semaphore_signal(
            barrier, inc=1, device_id={"space": lax.rem(here + step, spaces)}
        )

    @pl.when(core == 0)
    def _():
        pl.semaphore_signal(barrier, inc=1, device_id={"spin": 1 - core})

    if relayed:
        for g in range(groups):
            for number in range(moments):

                @pl.when(here == 0)
                def _(g=g, number=number):
                    chunk_recv[number, g, 0] = jnp.zeros_like(chunk_recv[number, g, 0])

                @pl.when(here == last)
                def _(g=g, number=number):
                    chunk_recv[number, g, last - 1] = jnp.zeros_like(chunk_recv[number, g, 0])

    for load in loads[:2]:
        load.wait()
    for mu in range(3):
        for c in range(3):
            for d in range(3):
                row = ((mu * 3 + c) * 3 + d) * 2
                links[row : row + 2, :] = link_ref[mu, c, d].astype(jnp.float32)

    def link(mu, c, d):
        row = ((mu * 3 + c) * 3 + d) * 2
        return [
            jnp.broadcast_to(links[row + part : row + part + 1, :], (GROUP, plane))
            for part in range(2)
        ]

    def colour(mu, half, dagger):
        outs = [[None] * 3 for _ in range(2)]
        for c in range(3):
            for d in range(3):
                u_real, u_imag = link(mu, d, c) if dagger else link(mu, c, d)
                for spin in range(2):
                    v_real, v_imag = half[spin][d]
                    if dagger:
                        real = u_real * v_real + u_imag * v_imag
                        imag = u_real * v_imag - u_imag * v_real
                    else:
                        real = u_real * v_real - u_imag * v_imag
                        imag = u_real * v_imag + u_imag * v_real
                    held = outs[spin][c]
                    outs[spin][c] = (
                        (real, imag) if held is None else (held[0] + real, held[1] + imag)
                    )
        return outs

    lanes = lax.broadcasted_iota(jnp.int32, (GROUP, plane), 1)
    column_x = lax.rem(lanes, width_x)

    def rolled(value, steps, along_y):
        if along_y:
            return pltpu.roll(value, (steps * width_x) % plane, 1)
        plain = pltpu.roll(value, steps % plane, 1)
        wrapped = pltpu.roll(value, (steps - steps * width_x) % plane, 1)
        edge = 0 if steps == 1 else width_x - 1
        return jnp.where(column_x == edge, wrapped, plain)

    def rolled_half(half, steps, along_y):
        return [
            [tuple(rolled(part, steps, along_y) for part in value) for value in spin]
            for spin in half
        ]

    def spinor(cols):
        return [
            [
                tuple(fwd_ref[part, s, c, cols, :].astype(jnp.float32) for part in range(2))
                for c in range(3)
            ]
            for s in range(4)
        ]

    def group(index):
        if isinstance(index, int):
            return slice(index * GROUP, (index + 1) * GROUP)
        return pl.ds(pl.multiple_of(index * GROUP, GROUP), GROUP)

    def halo_copy(g, side):
        return pltpu.make_async_remote_copy(
            src_ref=halo_send.at[g, side],
            dst_ref=halo_recv.at[g, side],
            send_sem=halo_send_sem,
            recv_sem=halo_recv_sems.at[g],
            device_id={"space": before if side == 0 else after},
        )

    for g in range(groups):
        psi = spinor(group(g))
        turned = small_times(singles[2][:2, 2:], psi[2:])
        minus = subtracted(psi[:2], turned)
        plus = colour(2, added(psi[:2], turned), True)
        for side, half in enumerate((minus, plus)):
            for spin in range(2):
                for c in range(3):
                    for part in range(2):
                        halo_send[g, side, part, spin, c] = half[spin][c][part].astype(
                            jnp.bfloat16
                        )
        if g == 0:
            pl.semaphore_wait(barrier, last + core)

        pl.when(here != last)(halo_copy(g, 0).start)
        pl.when(here != 0)(halo_copy(g, 1).start)
    for g in range(groups):
        pl.when(here == last)(halo_copy(g, 0).start)
        pl.when(here == 0)(halo_copy(g, 1).start)

    loads[2].wait()
    back_copy = pltpu.make_async_remote_copy(
        src_ref=back_ref,
        dst_ref=other_back,
        send_sem=back_sems.at[0],
        recv_sem=back_sems.at[1],
        device_id={"spin": 1 - core},
    )

    @pl.when(core == 1)
    def _():
        pl.semaphore_signal(ready_sem, inc=1, device_id={"spin": 1 - core})
        back_copy.start()

    def store_weave(cols, full, first):
        for s in range(4):
            for c in range(3):
                for part in range(2):
                    value = full[s][c][part]
                    if not first:
                        value = value + weave[part, s, c, cols, :]
                    weave[part, s, c, cols, :] = value

    def plane_group(index, carry):
        cols = group(index)
        psi = spinor(cols)
        upper = lower = None
        for mu in range(2):
            turned = small_times(singles[mu][:2, 2:], psi[2:])
            ahead = colour(mu, rolled_half(subtracted(psi[:2], turned), -1, mu == 1), False)
            behind = rolled_half(colour(mu, added(psi[:2], turned), True), 1, mu == 1)
            up = subtracted(ahead, behind)
            low = small_times(-singles[mu][2:, :2], added(ahead, behind))
            upper = up if upper is None else added(upper, up)
            lower = low if lower is None else added(lower, low)
        store_weave(cols, upper + lower, True)
        return carry

    lax.fori_loop(0, groups, plane_group, 0)

    for load in loads[3:]:
        load.wait()
    sites = lax.broadcasted_iota(jnp.int32, (8, plane), 1)
    coord_x = lax.rem(sites, width_x).astype(jnp.float32)
    coord_y = lax.div(sites, width_x).astype(jnp.float32)
    coord_z = here.astype(jnp.float32)
    phases = []
    for number in range(moments):
        momentum = [momenta_ref[number, axis].astype(jnp.float32) for axis in range(3)]
        turns = coord_x * (momentum[0] * (1.0 / width_x))
        turns = turns + coord_y * (momentum[1] * (width_x / plane))
        turns = turns + coord_z * (momentum[2] * (1.0 / full_z))
        theta = (2.0 * math.pi) * (turns - jnp.floor(turns))
        phases.append((jnp.cos(theta)[:1, :], jnp.sin(theta)[:1, :]))

    def arrange(owner, source):
        for part in range(2):
            for c in range(3):
                lane = (part * 3 + c) * plane
                for s in range(4):
                    for j in range(columns // rows):
                        row = (j * 4 + s) * rows
                        rows_scr[owner, row : row + rows, lane : lane + plane] = source[
                            part, s, c, j * rows : (j + 1) * rows, :
                        ]

    arrange(core, back_ref)

    @pl.when(core == 0)
    def _():
        pl.semaphore_wait(ready_sem, 1)
        back_copy.start()

    back_copy.wait_recv()
    arrange(1 - core, other_back)

    inner = (here != 0) & (here != last)
    far = jnp.where(here == 1, last, 0)

    def chunk_copy(g, number, step, relay=False):
        owner = lax.rem(here + step, spaces)
        if relay:
            target = last - 1 if step == 1 else 1
            target_ref, recv_sem = relay_recv.at[g, number], relay_sems.at[g, number]
        else:
            target = owner
            target_ref, recv_sem = chunk_recv.at[number, g, step - 1], chunk_recv_sems.at[number]
        return pltpu.make_async_remote_copy(
            src_ref=chunk_send.at[g, number, owner],
            dst_ref=target_ref,
            send_sem=chunk_send_sem,
            recv_sem=recv_sem,
            device_id={"space": target},
        )

    def wait_all(ref, send_sem, recv_sem):
        copy = pltpu.make_async_remote_copy(
            src_ref=ref,
            dst_ref=ref,
            send_sem=send_sem,
            recv_sem=recv_sem,
            device_id={"space": after},
        )
        return copy

    def wait_chunks(number):
        def wait(first, end):
            ref = chunk_recv.at[number, :, first:end]
            wait_all(ref, chunk_send_sem, chunk_recv_sems.at[number]).wait_recv()

        if not relayed:
            wait(0, last)
            return
        pl.when(inner)(functools.partial(wait, 0, last))
        pl.when(here == 0)(functools.partial(wait, 1, last))
        pl.when(here == last)(functools.partial(wait, 0, last - 1))

    chunk_rows = 4 * rows
    order = sorted(range(1, spaces), key=lambda step: -min(step, spaces - step))
    def depth_group(g):
        wait_all(halo_recv.at[g], halo_send_sem, halo_recv_sems.at[g]).wait_recv()
        received = [
            [
                [
                    tuple(
                        halo_recv[g, side, part, spin, c].astype(jnp.float32)
                        for part in range(2)
                    )
                    for c in range(3)
                ]
                for spin in range(2)
            ]
            for side in range(2)
        ]
        ahead = colour(2, received[0], False)
        behind = received[1]
        upper = subtracted(ahead, behind)
        lower = small_times(-singles[2][2:, :2], added(ahead, behind))
        store_weave(group(g), upper + lower, False)

    def rotate(g, number, dot, top):
        cols = group(g)
        cosine, sine = phases[number]
        for s in range(4):
            for c in range(3):
                real = weave[0, s, c, cols, :]
                imag = weave[1, s, c, cols, :]
                turned_real = (cosine * real + sine * imag).astype(jnp.bfloat16)
                turned_imag = (cosine * imag - sine * real).astype(jnp.bfloat16)
                at = top + 2 * s * GROUP
                rows_at = slice(at, at + GROUP)
                rows_next = slice(at + GROUP, at + 2 * GROUP)
                lanes_at = slice(c * plane, (c + 1) * plane)
                lanes_next = slice((3 + c) * plane, (4 + c) * plane)
                weave_mm[dot, rows_at, lanes_at] = turned_real
                weave_mm[dot, rows_at, lanes_next] = turned_imag
                weave_mm[dot, rows_next, lanes_at] = turned_imag
                weave_mm[dot, rows_next, lanes_next] = -turned_real

    def send_first(g, number):
        if not relayed:
            for step in order:
                chunk_copy(g, number, step).start()
            return
        for step in (1, last):
            pl.when(inner)(chunk_copy(g, number, step).start)
            end = last if step == 1 else 0
            pl.when(here == end)(chunk_copy(g, number, step, True).start)

    def send_rest(g, number, phase):
        if phase == 0:
            for step in range(2, last):
                delayed = inner & (lax.rem(here + step, spaces) == far)
                pl.when(jnp.logical_not(delayed))(chunk_copy(g, number, step).start)
        else:
            for step in (1, last):
                first = inner | (here == (last if step == 1 else 0))
                pl.when(jnp.logical_not(first))(chunk_copy(g, number, step).start)

    width = pair.shape[-1]
    pieces = [(g, number) for g in range(groups) for number in range(moments)]
    ready = 0
    for dot in range((len(pieces) + 1) // 2):
        inside = pieces[2 * dot : 2 * dot + 2]
        while ready <= inside[-1][0]:
            depth_group(ready)
            ready += 1
        for index, (g, number) in enumerate(inside):
            rotate(g, number, dot, index * width)
        product = lax.dot_general(
            rows_scr[...].reshape(8 * columns, 6 * plane),
            weave_mm[dot, : len(inside) * width],
            (((1,), (1,)), ((), ())),
            preferred_element_type=jnp.float32,
        )
        for index, (g, number) in enumerate(inside):
            for target in range(spaces):
                piece = product[
                    target * chunk_rows : (target + 1) * chunk_rows,
                    index * width : (index + 1) * width,
                ]
                pair[g, number, target] = piece
                chunk_send[g, number, target] = piece.astype(jnp.bfloat16)
            send_first(g, number)
    if relayed:
        for phase in range(2):
            for g, number in pieces:
                send_rest(g, number, phase)

    if relayed:
        for g in range(groups):
            for number in range(moments):
                for step in range(2, last):

                    @pl.when(((here == 1) & (step == last - 1)) | ((here == last - 1) & (step == 2)))
                    def _(g=g, number=number, step=step):
                        chunk_copy(g, number, last, True).wait_recv()
                        target = lax.rem(here + step, spaces)
                        summed = pair[g, number, target] + relay_recv[g, number].astype(
                            jnp.float32
                        )
                        chunk_send[g, number, target] = summed.astype(jnp.bfloat16)
                        chunk_copy(g, number, step).start()

    def summed_piece(g, number):
        total = pair[g, number, here]
        for step in range(1, spaces):
            total = total + chunk_recv[number, g, step - 1].astype(jnp.float32)
        return total * scaling

    lane = lax.broadcasted_iota(jnp.int32, (rows, width), 1)
    slot = lax.div(lax.rem(lane, groups * GROUP), GROUP)
    for number in range(moments):
        if number == moments - 1:
            back_copy.wait_send()
            wait_all(halo_send, halo_send_sem, halo_recv_sems.at[0]).wait_send()
            sent = chunk_send.at[:, :, :last]
            wait_all(sent, chunk_send_sem, chunk_recv_sems.at[0]).wait_send()
        wait_chunks(number)
        totals = [summed_piece(g, number) for g in range(groups)]
        for s in range(4):
            for part in range(2):
                merged = None
                for g in range(groups):
                    value = totals[g][s * rows : (s + 1) * rows]
                    if g != part:
                        value = pltpu.roll(value, (width + (g - part) * GROUP) % width, 1)
                    merged = value if merged is None else jnp.where(slot == g, value, merged)
                for t in range(4):
                    value = merged
                    if t:
                        value = pltpu.roll(merged, width - t * 2 * GROUP, 1)
                    folded[(2 * part * 4 + s) * 4 + t, number] = value
                    folded[((2 * part + 1) * 4 + s) * 4 + t, number] = -value
        for k in range(gammas):
            for part in range(2):
                picks = [table_ref[gamma_ref[k], part * 4 + s] for s in range(4)]
                value = folded[picks[0], number] + folded[picks[1], number]
                value = value + (folded[picks[2], number] + folded[picks[3], number])
                out_ref[part, number, k] = value[:, :columns]


def store_kernel(value_ref, out_hbm, sems):
    moments = value_ref.shape[1]
    stores = [
        pltpu.make_async_copy(
            value_ref.at[:, number], out_hbm.at[:, number], sems.at[number]
        )
        for number in range(moments)
    ]
    for store in stores:
        store.start()
    for store in stores:
        store.wait()


def body(mesh, backward, forward, gauge_links, momenta, gamma_list):
    spaces = mesh.shape["space"]
    _, times, _, columns, _, layers, plane = forward.shape
    moments = momenta.shape[0]
    gammas = gamma_list.shape[0]
    rows = columns * mesh.shape["spin"] // spaces
    groups = columns // GROUP
    back = jnp.transpose(backward, (0, 1, 2, 4, 5, 3, 6)).reshape(2, 4, 3, columns, plane)
    fwd = jnp.transpose(forward, (0, 1, 2, 4, 5, 3, 6)).reshape(2, 4, 3, columns, plane)
    link = jnp.transpose(gauge_links, (1, 2, 3, 4, 5, 0, 6)).reshape(3, 3, 3, 2, plane)
    full_z = layers * spaces
    scaling = 0.5 / math.sqrt(3.0 * plane * full_z)
    _, basis = gamma_tables()
    table = pick_table(basis)
    width = 8 * GROUP
    vmem = pl.BlockSpec(memory_space=pltpu.VMEM)
    anywhere = pl.BlockSpec(memory_space=pl.ANY)
    out_shape = (2, moments, gammas, rows, columns)
    values = pl.pallas_call(
        functools.partial(kernel, spaces, LX, full_z, scaling),
        out_shape=pltpu.VMEM(out_shape, jnp.float32),
        in_specs=[anywhere] * 6,
        out_specs=vmem,
        scratch_shapes=[
            pltpu.VMEM(back.shape, back.dtype),
            pltpu.VMEM(fwd.shape, fwd.dtype),
            pltpu.VMEM(link.shape, link.dtype),
            pltpu.SMEM(table.shape, table.dtype),
            pltpu.SMEM(momenta.shape, momenta.dtype),
            pltpu.SMEM(gamma_list.shape, gamma_list.dtype),
            pltpu.VMEM((2, 4, 3, columns, plane), jnp.bfloat16),
            pltpu.VMEM((64, moments, rows, width), jnp.float32),
            pltpu.VMEM((56, plane), jnp.float32),
            pltpu.VMEM((groups, 2, 2, 2, 3, GROUP, plane), jnp.bfloat16),
            pltpu.VMEM((groups, 2, 2, 2, 3, GROUP, plane), jnp.bfloat16),
            pltpu.VMEM((2, 4 * columns, 6 * plane), jnp.bfloat16),
            pltpu.VMEM((2, 4, 3, columns, plane), jnp.float32),
            pltpu.VMEM(((groups * moments + 1) // 2, 2 * width, 6 * plane), jnp.bfloat16),
            pltpu.VMEM((groups, moments, spaces, 4 * rows, width), jnp.float32),
            pltpu.VMEM((groups, moments, spaces, 4 * rows, width), jnp.bfloat16),
            pltpu.VMEM((moments, groups, spaces - 1, 4 * rows, width), jnp.bfloat16),
            pltpu.VMEM((groups, moments, 4 * rows, width), jnp.bfloat16),
            pltpu.SemaphoreType.DMA((6,)),
            pltpu.SemaphoreType.DMA((2,)),
            pltpu.SemaphoreType.DMA,
            pltpu.SemaphoreType.DMA((groups,)),
            pltpu.SemaphoreType.DMA,
            pltpu.SemaphoreType.DMA((moments,)),
            pltpu.SemaphoreType.DMA((groups, moments)),
            pltpu.SemaphoreType.REGULAR,
        ],
        compiler_params=pltpu.CompilerParams(collective_id=0, has_side_effects=True),
    )(back, fwd, link, momenta, gamma_list, table)
    out = pl.pallas_call(
        store_kernel,
        out_shape=jax.ShapeDtypeStruct(out_shape, jnp.float32),
        in_specs=[vmem],
        out_specs=anywhere,
        scratch_shapes=[pltpu.SemaphoreType.DMA((moments,))],
    )(pltpu.with_memory_space_constraint(values, pltpu.VMEM))
    return out.reshape(2, moments, gammas, times, rows, columns)


def solution(mesh):
    in_specs = (
        P("parts", "tm", None, "spin", None, "space", None),
        P("parts", "tm", None, "spin", None, "space", None),
        P("parts", None, None, None, "tm", "space", None),
        P(),
        P(),
    )
    out_specs = P("parts", None, None, "tm", "space", "spin")
    return jax.shard_map(
        functools.partial(body, mesh),
        mesh=mesh,
        in_specs=in_specs,
        out_specs=out_specs,
        check_vma=False,
    )
```

```python
import functools
import math

import jax
import jax.numpy as jnp
import numpy as np
from jax import lax
from jax.experimental import pallas as pl
from jax.experimental.pallas import tpu as pltpu
from jax.sharding import PartitionSpec as P

LX = 32
GROUP = 16
LINE = 4


def gamma_tables():
    zeros = np.zeros((4, 4))
    gx_imag = np.array([[0, 0, 0, 1], [0, 0, 1, 0], [0, -1, 0, 0], [-1, 0, 0, 0]]) * 1.0
    gy_real = np.array([[0, 0, 0, -1], [0, 0, 1, 0], [0, 1, 0, 0], [-1, 0, 0, 0]]) * 1.0
    gz_imag = np.array([[0, 0, 1, 0], [0, 0, 0, -1], [-1, 0, 0, 0], [0, 1, 0, 0]]) * 1.0
    gt_real = np.array([[0, 0, 1, 0], [0, 0, 0, 1], [1, 0, 0, 0], [0, 1, 0, 0]]) * 1.0
    singles = [zeros + 1j * gx_imag, gy_real + 0j, 1j * gz_imag, gt_real + 0j]
    basis = []
    for number in range(16):
        matrix = np.eye(4) + 0j
        for which in range(4):
            if number >> which & 1:
                matrix = matrix @ singles[which]
        basis.append(matrix)
    return singles, np.stack(basis)


def picked(units, part):
    if all(unit.imag == 0 for unit in units):
        return part, [int(unit.real) for unit in units]
    assert all(unit.real == 0 for unit in units)
    sign = -1 if part == 0 else 1
    return 1 - part, [sign * int(unit.imag) for unit in units]


def signed_sum(first_sign, first, second_sign, second):
    if first_sign > 0:
        return first + second if second_sign > 0 else first - second
    return second - first if second_sign > 0 else -first - second


def unit_times(unit, value):
    real, imag = value
    if unit == 1:
        return real, imag
    if unit == -1:
        return -real, -imag
    if unit == 1j:
        return -imag, real
    return imag, -real


def small_times(matrix, half):
    outs = []
    for row in range(2):
        column = int(np.flatnonzero(matrix[row])[0])
        outs.append([unit_times(complex(matrix[row, column]), value) for value in half[column]])
    return outs


def added(first, second):
    return [
        [(a[0] + b[0], a[1] + b[1]) for a, b in zip(left, right)]
        for left, right in zip(first, second)
    ]


def subtracted(first, second):
    return [
        [(a[0] - b[0], a[1] - b[1]) for a, b in zip(left, right)]
        for left, right in zip(first, second)
    ]


def kernel(
    spaces,
    width_x,
    full_z,
    scaling,
    back_hbm,
    fwd_hbm,
    link_hbm,
    momenta_hbm,
    gamma_hbm,
    out_ref,
    back_ref,
    fwd_ref,
    link_ref,
    momenta_ref,
    gamma_ref,
    other_back,
    results,
    links,
    halo_send,
    halo_recv,
    rows_scr,
    weave,
    weave_mm,
    pair,
    chunk_send,
    far_send,
    chunk_recv,
    relay_recv,
    load_sems,
    back_sems,
    halo_send_sem,
    halo_recv_sems,
    chunk_send_sem,
    chunk_recv_sems,
    relay_sems,
    ready_sem,
    turn_sem,
):
    loads = [
        pltpu.make_async_copy(source, target, load_sems.at[number])
        for number, (source, target) in enumerate(
            (
                (fwd_hbm, fwd_ref),
                (link_hbm, link_ref),
                (back_hbm, back_ref),
                (momenta_hbm, momenta_ref),
                (gamma_hbm, gamma_ref),
            )
        )
    ]
    for load in loads:
        load.start()
    columns = fwd_ref.shape[3]
    plane = fwd_ref.shape[4]
    moments = momenta_ref.shape[0]
    gammas = gamma_ref.shape[0]
    groups = columns // GROUP
    rows = columns * 2 // spaces
    last = spaces - 1
    relayed = 4 <= spaces <= LINE
    here = lax.axis_index("space")
    core = lax.axis_index("spin")
    after = lax.rem(here + 1, spaces)
    before = lax.rem(here + last, spaces)
    singles, basis = gamma_tables()

    barrier = pltpu.get_barrier_semaphore()
    if relayed:
        greeted = 2
        for target in (before, after):
            pl.semaphore_signal(barrier, inc=1, device_id={"space": target})
    else:
        greeted = last
        for step in range(1, spaces):
            target = lax.rem(here + step, spaces)
            pl.semaphore_signal(barrier, inc=1, device_id={"space": target})

    @pl.when(core == 0)
    def _():
        pl.semaphore_signal(barrier, inc=1, device_id={"spin": 1 - core})

    if relayed:
        for g in range(groups):
            for number in range(moments):

                @pl.when(here == 0)
                def _(g=g, number=number):
                    chunk_recv[number, g, 0] = jnp.zeros_like(chunk_recv[number, g, 0])

                @pl.when(here == last)
                def _(g=g, number=number):
                    chunk_recv[number, g, last - 1] = jnp.zeros_like(chunk_recv[number, g, 0])

    for load in loads[:2]:
        load.wait()
    for mu in range(3):
        for c in range(3):
            for d in range(3):
                row = ((mu * 3 + c) * 3 + d) * 2
                links[row : row + 2, :] = link_ref[mu, c, d].astype(jnp.float32)

    def link(mu, c, d):
        row = ((mu * 3 + c) * 3 + d) * 2
        return [
            jnp.broadcast_to(links[row + part : row + part + 1, :], (GROUP, plane))
            for part in range(2)
        ]

    def colour(mu, half, dagger):
        outs = [[None] * 3 for _ in range(2)]
        for c in range(3):
            for d in range(3):
                u_real, u_imag = link(mu, d, c) if dagger else link(mu, c, d)
                for spin in range(2):
                    v_real, v_imag = half[spin][d]
                    if dagger:
                        real = u_real * v_real + u_imag * v_imag
                        imag = u_real * v_imag - u_imag * v_real
                    else:
                        real = u_real * v_real - u_imag * v_imag
                        imag = u_real * v_imag + u_imag * v_real
                    held = outs[spin][c]
                    outs[spin][c] = (
                        (real, imag) if held is None else (held[0] + real, held[1] + imag)
                    )
        return outs

    lanes = lax.broadcasted_iota(jnp.int32, (GROUP, plane), 1)
    column_x = lax.rem(lanes, width_x)

    def rolled(value, steps, along_y):
        if along_y:
            return pltpu.roll(value, (steps * width_x) % plane, 1)
        plain = pltpu.roll(value, steps % plane, 1)
        wrapped = pltpu.roll(value, (steps - steps * width_x) % plane, 1)
        edge = 0 if steps == 1 else width_x - 1
        return jnp.where(column_x == edge, wrapped, plain)

    def rolled_half(half, steps, along_y):
        return [
            [tuple(rolled(part, steps, along_y) for part in value) for value in spin]
            for spin in half
        ]

    def spinor(cols):
        return [
            [
                tuple(fwd_ref[part, s, c, cols, :].astype(jnp.float32) for part in range(2))
                for c in range(3)
            ]
            for s in range(4)
        ]

    def group(index):
        if isinstance(index, int):
            return slice(index * GROUP, (index + 1) * GROUP)
        return pl.ds(pl.multiple_of(index * GROUP, GROUP), GROUP)

    def halo_copy(g, side):
        return pltpu.make_async_remote_copy(
            src_ref=halo_send.at[g, side],
            dst_ref=halo_recv.at[g, side],
            send_sem=halo_send_sem,
            recv_sem=halo_recv_sems.at[g],
            device_id={"space": before if side == 0 else after},
        )

    for g in range(groups):
        psi = spinor(group(g))
        turned = small_times(singles[2][:2, 2:], psi[2:])
        minus = subtracted(psi[:2], turned)
        plus = colour(2, added(psi[:2], turned), True)
        for side, half in enumerate((minus, plus)):
            for spin in range(2):
                for c in range(3):
                    for part in range(2):
                        halo_send[g, side, part, spin, c] = half[spin][c][part].astype(
                            jnp.bfloat16
                        )
        if g == 0:
            pl.semaphore_wait(barrier, greeted + core)

        pl.when(here != last)(halo_copy(g, 0).start)
        pl.when(here != 0)(halo_copy(g, 1).start)
    for g in range(groups):
        pl.when(here == last)(halo_copy(g, 0).start)
        pl.when(here == 0)(halo_copy(g, 1).start)

    loads[2].wait()
    back_copy = pltpu.make_async_remote_copy(
        src_ref=back_ref,
        dst_ref=other_back,
        send_sem=back_sems.at[0],
        recv_sem=back_sems.at[1],
        device_id={"spin": 1 - core},
    )

    @pl.when(core == 1)
    def _():
        pl.semaphore_signal(ready_sem, inc=1, device_id={"spin": 1 - core})
        back_copy.start()

    def store_weave(cols, full, first):
        for s in range(4):
            for c in range(3):
                for part in range(2):
                    value = full[s][c][part]
                    if not first:
                        value = value + weave[part, s, c, cols, :]
                    weave[part, s, c, cols, :] = value

    def plane_group(index, carry):
        cols = group(index)
        psi = spinor(cols)
        upper = lower = None
        for mu in range(2):
            turned = small_times(singles[mu][:2, 2:], psi[2:])
            ahead = colour(mu, rolled_half(subtracted(psi[:2], turned), -1, mu == 1), False)
            behind = rolled_half(colour(mu, added(psi[:2], turned), True), 1, mu == 1)
            up = subtracted(ahead, behind)
            low = small_times(-singles[mu][2:, :2], added(ahead, behind))
            upper = up if upper is None else added(upper, up)
            lower = low if lower is None else added(lower, low)
        store_weave(cols, upper + lower, True)
        return carry

    lax.fori_loop(0, groups, plane_group, 0)

    for load in loads[3:]:
        load.wait()
    sites = lax.broadcasted_iota(jnp.int32, (8, plane), 1)
    coord_x = lax.rem(sites, width_x).astype(jnp.float32)
    coord_y = lax.div(sites, width_x).astype(jnp.float32)
    coord_z = here.astype(jnp.float32)
    phases = []
    for number in range(moments):
        momentum = [momenta_ref[number, axis].astype(jnp.float32) for axis in range(3)]
        turns = coord_x * (momentum[0] * (1.0 / width_x))
        turns = turns + coord_y * (momentum[1] * (width_x / plane))
        turns = turns + coord_z * (momentum[2] * (1.0 / full_z))
        theta = (2.0 * math.pi) * (turns - jnp.floor(turns))
        phases.append((jnp.cos(theta)[:1, :], jnp.sin(theta)[:1, :]))

    def arrange(owner, source):
        for part in range(2):
            for c in range(3):
                lane = (part * 3 + c) * plane
                for s in range(4):
                    for j in range(columns // rows):
                        row = (j * 4 + s) * rows
                        rows_scr[owner, row : row + rows, lane : lane + plane] = source[
                            part, s, c, j * rows : (j + 1) * rows, :
                        ]

    arrange(core, back_ref)

    @pl.when(core == 0)
    def _():
        pl.semaphore_wait(ready_sem, 1)
        back_copy.start()

    back_copy.wait_recv()
    arrange(1 - core, other_back)

    inner = (here != 0) & (here != last)
    far = jnp.where(2 * here < spaces, last, 0)

    def chunk_copy(g, number, step, relay=False):
        owner = lax.rem(here + step, spaces)
        source_ref = chunk_send.at[g, number, owner]
        if relay:
            source_ref = far_send.at[g, number]
            target = last - 1 if step == 1 else 1
            target_ref, recv_sem = relay_recv.at[g, number], relay_sems.at[g, number]
        else:
            target = owner
            target_ref, recv_sem = chunk_recv.at[number, g, step - 1], chunk_recv_sems.at[number]
        return pltpu.make_async_remote_copy(
            src_ref=source_ref,
            dst_ref=target_ref,
            send_sem=chunk_send_sem,
            recv_sem=recv_sem,
            device_id={"space": target},
        )

    def wait_all(ref, send_sem, recv_sem):
        copy = pltpu.make_async_remote_copy(
            src_ref=ref,
            dst_ref=ref,
            send_sem=send_sem,
            recv_sem=recv_sem,
            device_id={"space": after},
        )
        return copy

    def wait_chunks(number):
        def wait(first, end):
            ref = chunk_recv.at[number, :, first:end]
            wait_all(ref, chunk_send_sem, chunk_recv_sems.at[number]).wait_recv()

        if not relayed:
            wait(0, last)
            return
        pl.when(inner)(functools.partial(wait, 0, last))
        pl.when(here == 0)(functools.partial(wait, 1, last))
        pl.when(here == last)(functools.partial(wait, 0, last - 1))

    chunk_rows = 4 * rows
    order = sorted(range(1, spaces), key=lambda step: -min(step, spaces - step))
    def depth_group(g):
        wait_all(halo_recv.at[g], halo_send_sem, halo_recv_sems.at[g]).wait_recv()
        received = [
            [
                [
                    tuple(
                        halo_recv[g, side, part, spin, c].astype(jnp.float32)
                        for part in range(2)
                    )
                    for c in range(3)
                ]
                for spin in range(2)
            ]
            for side in range(2)
        ]
        ahead = colour(2, received[0], False)
        behind = received[1]
        upper = subtracted(ahead, behind)
        lower = small_times(-singles[2][2:, :2], added(ahead, behind))
        store_weave(group(g), upper + lower, False)

    def rotate(g, number, dot, top):
        cols = group(g)
        cosine, sine = phases[number]
        for s in range(4):
            for c in range(3):
                real = weave[0, s, c, cols, :]
                imag = weave[1, s, c, cols, :]
                turned_real = (cosine * real + sine * imag).astype(jnp.bfloat16)
                turned_imag = (cosine * imag - sine * real).astype(jnp.bfloat16)
                at = top + 2 * s * GROUP
                rows_at = slice(at, at + GROUP)
                rows_next = slice(at + GROUP, at + 2 * GROUP)
                lanes_at = slice(c * plane, (c + 1) * plane)
                lanes_next = slice((3 + c) * plane, (4 + c) * plane)
                weave_mm[dot, rows_at, lanes_at] = turned_real
                weave_mm[dot, rows_at, lanes_next] = turned_imag
                weave_mm[dot, rows_next, lanes_at] = turned_imag
                weave_mm[dot, rows_next, lanes_next] = -turned_real

    def send_far(g, number):
        pl.when(here == last)(chunk_copy(g, number, 1, True).start)
        pl.when(here == 0)(chunk_copy(g, number, last, True).start)

    def send_first(g, number):
        if not relayed:
            for step in order:
                chunk_copy(g, number, step).start()
            return
        for step in (1, last):
            pl.when(inner)(chunk_copy(g, number, step).start)

    def send_rest(those):
        for step in range(2, last):
            delayed = inner & (lax.rem(here + step, spaces) == far)
            for g in those:
                for number in range(moments):
                    pl.when(jnp.logical_not(delayed))(chunk_copy(g, number, step).start)
        for step in (1, last):
            near = here == (0 if step == 1 else last)
            for g in those:
                for number in range(moments):
                    pl.when(near)(chunk_copy(g, number, step).start)

    width = pair.shape[-1]

    def product(g, rows_in):
        return lax.dot_general(
            rows_in, weave_mm[g], (((1,), (1,)), ((), ())), preferred_element_type=jnp.float32
        )

    far_owner = lax.div(far * rows, columns)
    far_row = pl.multiple_of(lax.rem(far * 4 * rows, 4 * columns), chunk_rows)
    for g in range(groups):
        depth_group(g)
        for number in range(moments):
            rotate(g, number, g, number * width)
        if relayed:
            value = product(g, rows_scr[far_owner, pl.ds(far_row, chunk_rows), :])
            for number in range(moments):
                piece = value[:, number * width : (number + 1) * width]
                far_send[g, number] = piece.astype(jnp.bfloat16)
                send_far(g, number)
            if g == groups - 1:

                @pl.when((core == 0) & jnp.logical_not(inner))
                def _():
                    pl.semaphore_signal(turn_sem, inc=1, device_id={"spin": 1 - core})

        value = product(g, rows_scr[...].reshape(8 * columns, 6 * plane))
        for number in range(moments):
            for owner in range(spaces):
                piece = value[
                    owner * chunk_rows : (owner + 1) * chunk_rows,
                    number * width : (number + 1) * width,
                ]
                pair[g, number, owner] = piece
                chunk_send[g, number, owner] = piece.astype(jnp.bfloat16)
            send_first(g, number)
        if relayed and g < groups - 1:
            pl.when((core == 1) & jnp.logical_not(inner))(
                functools.partial(send_rest, range(g, g + 1))
            )
    if relayed:
        @pl.when((core == 1) & jnp.logical_not(inner))
        def _():
            pl.semaphore_wait(turn_sem, 1)
            send_rest(range(groups - 1, groups))

        @pl.when((core == 0) | inner)
        def _():
            send_rest(range(groups))

    if relayed:
        for g in range(groups):
            for number in range(moments):
                for step in range(2, last):

                    @pl.when(((here == 1) & (step == last - 1)) | ((here == last - 1) & (step == 2)))
                    def _(g=g, number=number, step=step):
                        chunk_copy(g, number, last, True).wait_recv()
                        target = lax.rem(here + step, spaces)
                        summed = pair[g, number, target] + relay_recv[g, number].astype(
                            jnp.float32
                        )
                        chunk_send[g, number, target] = summed.astype(jnp.bfloat16)
                        chunk_copy(g, number, step).start()

    def summed_piece(g, number):
        total = pair[g, number, here]
        for step in range(1, spaces):
            total = total + chunk_recv[number, g, step - 1].astype(jnp.float32)
        return total * scaling

    lane = lax.broadcasted_iota(jnp.int32, (rows, width), 1)
    slot = lax.div(lax.rem(lane, groups * GROUP), GROUP)
    back_copy.wait_send()
    wait_all(halo_send, halo_send_sem, halo_recv_sems.at[0]).wait_send()
    wait_all(chunk_send.at[:, :, :last], chunk_send_sem, chunk_recv_sems.at[0]).wait_send()
    for number in range(moments):
        if number == 0:
            wait_chunks(0)
        elif number == 1:
            for other in range(1, moments):
                wait_chunks(other)
        totals = [summed_piece(g, number) for g in range(groups)]
        parts = []
        for part in range(2):
            merged_rows = []
            for s in range(4):
                merged = None
                for g in range(groups):
                    value = totals[g][s * rows : (s + 1) * rows]
                    if g != part:
                        value = pltpu.roll(value, (width + (g - part) * GROUP) % width, 1)
                    merged = value if merged is None else jnp.where(slot == g, value, merged)
                merged_rows.append(merged)
            parts.append(merged_rows)
        for offset in range(4):
            sums = []
            for part in range(2):
                terms = []
                for s in range(4):
                    t = s ^ offset
                    value = parts[part][s]
                    terms.append(pltpu.roll(value, width - t * 2 * GROUP, 1) if t else value)
                sums.append(
                    {
                        (pair_at, sign): terms[pair_at] + terms[pair_at + 1]
                        if sign > 0
                        else terms[pair_at] - terms[pair_at + 1]
                        for pair_at in (0, 2)
                        for sign in (1, -1)
                    }
                )
            for index in range(len(basis)):
                if np.flatnonzero(basis[index][0])[0] != offset:
                    continue
                units = [complex(basis[index][s, s ^ offset]) for s in range(4)]
                for part in range(2):
                    source, signs = picked(units, part)
                    first = sums[source][0, signs[0] * signs[1]]
                    second = sums[source][2, signs[2] * signs[3]]
                    results[number, index, part] = signed_sum(signs[0], first, signs[2], second)
        for k in range(gammas):
            for part in range(2):
                out_ref[part, number, k] = results[number, gamma_ref[k], part][:, :columns]


def store_kernel(value_ref, out_hbm, sems):
    moments = value_ref.shape[1]
    stores = [
        pltpu.make_async_copy(
            value_ref.at[:, number], out_hbm.at[:, number], sems.at[number]
        )
        for number in range(moments)
    ]
    for store in stores:
        store.start()
    for store in stores:
        store.wait()


def body(mesh, backward, forward, gauge_links, momenta, gamma_list):
    spaces = mesh.shape["space"]
    _, times, _, columns, _, layers, plane = forward.shape
    moments = momenta.shape[0]
    gammas = gamma_list.shape[0]
    rows = columns * mesh.shape["spin"] // spaces
    groups = columns // GROUP
    back = jnp.transpose(backward, (0, 1, 2, 4, 5, 3, 6)).reshape(2, 4, 3, columns, plane)
    fwd = jnp.transpose(forward, (0, 1, 2, 4, 5, 3, 6)).reshape(2, 4, 3, columns, plane)
    link = jnp.transpose(gauge_links, (1, 2, 3, 4, 5, 0, 6)).reshape(3, 3, 3, 2, plane)
    full_z = layers * spaces
    scaling = 0.5 / math.sqrt(3.0 * plane * full_z)
    width = 8 * GROUP
    vmem = pl.BlockSpec(memory_space=pltpu.VMEM)
    anywhere = pl.BlockSpec(memory_space=pl.ANY)
    out_shape = (2, moments, gammas, rows, columns)
    values = pl.pallas_call(
        functools.partial(kernel, spaces, LX, full_z, scaling),
        out_shape=pltpu.VMEM(out_shape, jnp.float32),
        in_specs=[anywhere] * 5,
        out_specs=vmem,
        scratch_shapes=[
            pltpu.VMEM(back.shape, back.dtype),
            pltpu.VMEM(fwd.shape, fwd.dtype),
            pltpu.VMEM(link.shape, link.dtype),
            pltpu.SMEM(momenta.shape, momenta.dtype),
            pltpu.SMEM(gamma_list.shape, gamma_list.dtype),
            pltpu.VMEM((2, 4, 3, columns, plane), jnp.bfloat16),
            pltpu.VMEM((moments, 16, 2, rows, width), jnp.float32),
            pltpu.VMEM((56, plane), jnp.float32),
            pltpu.VMEM((groups, 2, 2, 2, 3, GROUP, plane), jnp.bfloat16),
            pltpu.VMEM((groups, 2, 2, 2, 3, GROUP, plane), jnp.bfloat16),
            pltpu.VMEM((2, 4 * columns, 6 * plane), jnp.bfloat16),
            pltpu.VMEM((2, 4, 3, columns, plane), jnp.float32),
            pltpu.VMEM((groups, moments * width, 6 * plane), jnp.bfloat16),
            pltpu.VMEM((groups, moments, spaces, 4 * rows, width), jnp.float32),
            pltpu.VMEM((groups, moments, spaces, 4 * rows, width), jnp.bfloat16),
            pltpu.VMEM((groups, moments, 4 * rows, width), jnp.bfloat16),
            pltpu.VMEM((moments, groups, spaces - 1, 4 * rows, width), jnp.bfloat16),
            pltpu.VMEM((groups, moments, 4 * rows, width), jnp.bfloat16),
            pltpu.SemaphoreType.DMA((5,)),
            pltpu.SemaphoreType.DMA((2,)),
            pltpu.SemaphoreType.DMA,
            pltpu.SemaphoreType.DMA((groups,)),
            pltpu.SemaphoreType.DMA,
            pltpu.SemaphoreType.DMA((moments,)),
            pltpu.SemaphoreType.DMA((groups, moments)),
            pltpu.SemaphoreType.REGULAR,
            pltpu.SemaphoreType.REGULAR,
        ],
        compiler_params=pltpu.CompilerParams(collective_id=0, has_side_effects=True),
    )(back, fwd, link, momenta, gamma_list)
    out = pl.pallas_call(
        store_kernel,
        out_shape=jax.ShapeDtypeStruct(out_shape, jnp.float32),
        in_specs=[vmem],
        out_specs=anywhere,
        scratch_shapes=[pltpu.SemaphoreType.DMA((moments,))],
    )(pltpu.with_memory_space_constraint(values, pltpu.VMEM))
    return out.reshape(2, moments, gammas, times, rows, columns)


def solution(mesh):
    in_specs = (
        P("parts", "tm", None, "spin", None, "space", None),
        P("parts", "tm", None, "spin", None, "space", None),
        P("parts", None, None, None, "tm", "space", None),
        P(),
        P(),
    )
    out_specs = P("parts", None, None, "tm", "space", "spin")
    return jax.shard_map(
        functools.partial(body, mesh),
        mesh=mesh,
        in_specs=in_specs,
        out_specs=out_specs,
        check_vma=False,
    )
```

```python
import functools
import math

import jax
import jax.numpy as jnp
import numpy as np
from jax import lax
from jax.experimental import pallas as pl
from jax.experimental.pallas import tpu as pltpu
from jax.sharding import PartitionSpec as P

LX = 32
GROUP = 16
LINE = 4


def gamma_tables():
    zeros = np.zeros((4, 4))
    gx_imag = np.array([[0, 0, 0, 1], [0, 0, 1, 0], [0, -1, 0, 0], [-1, 0, 0, 0]]) * 1.0
    gy_real = np.array([[0, 0, 0, -1], [0, 0, 1, 0], [0, 1, 0, 0], [-1, 0, 0, 0]]) * 1.0
    gz_imag = np.array([[0, 0, 1, 0], [0, 0, 0, -1], [-1, 0, 0, 0], [0, 1, 0, 0]]) * 1.0
    gt_real = np.array([[0, 0, 1, 0], [0, 0, 0, 1], [1, 0, 0, 0], [0, 1, 0, 0]]) * 1.0
    singles = [zeros + 1j * gx_imag, gy_real + 0j, 1j * gz_imag, gt_real + 0j]
    basis = []
    for number in range(16):
        matrix = np.eye(4) + 0j
        for which in range(4):
            if number >> which & 1:
                matrix = matrix @ singles[which]
        basis.append(matrix)
    return singles, np.stack(basis)


def picked(units, part):
    if all(unit.imag == 0 for unit in units):
        return part, [int(unit.real) for unit in units]
    assert all(unit.real == 0 for unit in units)
    sign = -1 if part == 0 else 1
    return 1 - part, [sign * int(unit.imag) for unit in units]


def signed_sum(first_sign, first, second_sign, second):
    if first_sign > 0:
        return first + second if second_sign > 0 else first - second
    return second - first if second_sign > 0 else -first - second


def unit_times(unit, value):
    real, imag = value
    if unit == 1:
        return real, imag
    if unit == -1:
        return -real, -imag
    if unit == 1j:
        return -imag, real
    return imag, -real


def small_times(matrix, half):
    outs = []
    for row in range(2):
        column = int(np.flatnonzero(matrix[row])[0])
        outs.append([unit_times(complex(matrix[row, column]), value) for value in half[column]])
    return outs


def added(first, second):
    return [
        [(a[0] + b[0], a[1] + b[1]) for a, b in zip(left, right)]
        for left, right in zip(first, second)
    ]


def subtracted(first, second):
    return [
        [(a[0] - b[0], a[1] - b[1]) for a, b in zip(left, right)]
        for left, right in zip(first, second)
    ]


def kernel(
    spaces,
    width_x,
    full_z,
    scaling,
    back_hbm,
    fwd_hbm,
    link_hbm,
    momenta_hbm,
    gamma_hbm,
    out_ref,
    back_ref,
    fwd_ref,
    link_ref,
    momenta_ref,
    gamma_ref,
    other_back,
    results,
    links,
    halo_send,
    halo_recv,
    rows_scr,
    weave,
    weave_mm,
    pair,
    chunk_send,
    far_send,
    chunk_recv,
    relay_recv,
    load_sems,
    back_sems,
    halo_send_sem,
    halo_recv_sems,
    chunk_send_sem,
    chunk_recv_sems,
    relay_sems,
    ready_sem,
    turn_sem,
    near_sem,
):
    loads = [
        pltpu.make_async_copy(source, target, load_sems.at[number])
        for number, (source, target) in enumerate(
            (
                (fwd_hbm, fwd_ref),
                (link_hbm, link_ref),
                (back_hbm, back_ref),
                (momenta_hbm, momenta_ref),
                (gamma_hbm, gamma_ref),
            )
        )
    ]
    for load in loads:
        load.start()
    columns = fwd_ref.shape[3]
    plane = fwd_ref.shape[4]
    moments = momenta_ref.shape[0]
    gammas = gamma_ref.shape[0]
    groups = columns // GROUP
    rows = columns * 2 // spaces
    last = spaces - 1
    relayed = 4 <= spaces <= LINE
    here = lax.axis_index("space")
    core = lax.axis_index("spin")
    after = lax.rem(here + 1, spaces)
    before = lax.rem(here + last, spaces)
    singles, basis = gamma_tables()

    barrier = pltpu.get_barrier_semaphore()
    if relayed:
        greeted = 2
        for target in (before, after):
            pl.semaphore_signal(barrier, inc=1, device_id={"space": target})
    else:
        greeted = last
        for step in range(1, spaces):
            target = lax.rem(here + step, spaces)
            pl.semaphore_signal(barrier, inc=1, device_id={"space": target})

    @pl.when(core == 0)
    def _():
        pl.semaphore_signal(barrier, inc=1, device_id={"spin": 1 - core})

    if relayed:
        for g in range(groups):
            for number in range(moments):

                @pl.when(here == 0)
                def _(g=g, number=number):
                    chunk_recv[number, g, 0] = jnp.zeros_like(chunk_recv[number, g, 0])

                @pl.when(here == last)
                def _(g=g, number=number):
                    chunk_recv[number, g, last - 1] = jnp.zeros_like(chunk_recv[number, g, 0])

    for load in loads[:2]:
        load.wait()
    for mu in range(3):
        for c in range(3):
            for d in range(3):
                row = ((mu * 3 + c) * 3 + d) * 2
                links[row : row + 2, :] = link_ref[mu, c, d].astype(jnp.float32)

    def link(mu, c, d):
        row = ((mu * 3 + c) * 3 + d) * 2
        return [
            jnp.broadcast_to(links[row + part : row + part + 1, :], (GROUP, plane))
            for part in range(2)
        ]

    def colour(mu, half, dagger):
        outs = [[None] * 3 for _ in range(2)]
        for c in range(3):
            for d in range(3):
                u_real, u_imag = link(mu, d, c) if dagger else link(mu, c, d)
                for spin in range(2):
                    v_real, v_imag = half[spin][d]
                    if dagger:
                        real = u_real * v_real + u_imag * v_imag
                        imag = u_real * v_imag - u_imag * v_real
                    else:
                        real = u_real * v_real - u_imag * v_imag
                        imag = u_real * v_imag + u_imag * v_real
                    held = outs[spin][c]
                    outs[spin][c] = (
                        (real, imag) if held is None else (held[0] + real, held[1] + imag)
                    )
        return outs

    lanes = lax.broadcasted_iota(jnp.int32, (GROUP, plane), 1)
    column_x = lax.rem(lanes, width_x)

    def rolled(value, steps, along_y):
        if along_y:
            return pltpu.roll(value, (steps * width_x) % plane, 1)
        plain = pltpu.roll(value, steps % plane, 1)
        wrapped = pltpu.roll(value, (steps - steps * width_x) % plane, 1)
        edge = 0 if steps == 1 else width_x - 1
        return jnp.where(column_x == edge, wrapped, plain)

    def rolled_half(half, steps, along_y):
        return [
            [tuple(rolled(part, steps, along_y) for part in value) for value in spin]
            for spin in half
        ]

    def spinor(cols):
        return [
            [
                tuple(fwd_ref[part, s, c, cols, :].astype(jnp.float32) for part in range(2))
                for c in range(3)
            ]
            for s in range(4)
        ]

    def group(index):
        if isinstance(index, int):
            return slice(index * GROUP, (index + 1) * GROUP)
        return pl.ds(pl.multiple_of(index * GROUP, GROUP), GROUP)

    def halo_copy(g, side):
        return pltpu.make_async_remote_copy(
            src_ref=halo_send.at[g, side],
            dst_ref=halo_recv.at[g, side],
            send_sem=halo_send_sem,
            recv_sem=halo_recv_sems.at[g],
            device_id={"space": before if side == 0 else after},
        )

    for g in range(groups):
        psi = spinor(group(g))
        turned = small_times(singles[2][:2, 2:], psi[2:])
        minus = subtracted(psi[:2], turned)
        plus = colour(2, added(psi[:2], turned), True)
        for side, half in enumerate((minus, plus)):
            for spin in range(2):
                for c in range(3):
                    for part in range(2):
                        halo_send[g, side, part, spin, c] = half[spin][c][part].astype(
                            jnp.bfloat16
                        )
        if g == 0:
            pl.semaphore_wait(barrier, greeted + core)

        pl.when(here != last)(halo_copy(g, 0).start)
        pl.when(here != 0)(halo_copy(g, 1).start)
    for g in range(groups):
        pl.when(here == last)(halo_copy(g, 0).start)
        if relayed:
            pl.when((here == 0) & (core == 0))(halo_copy(g, 1).start)
        else:
            pl.when(here == 0)(halo_copy(g, 1).start)

    loads[2].wait()
    back_copy = pltpu.make_async_remote_copy(
        src_ref=back_ref,
        dst_ref=other_back,
        send_sem=back_sems.at[0],
        recv_sem=back_sems.at[1],
        device_id={"spin": 1 - core},
    )

    @pl.when(core == 1)
    def _():
        pl.semaphore_signal(ready_sem, inc=1, device_id={"spin": 1 - core})
        back_copy.start()

    def store_weave(cols, full, first):
        for s in range(4):
            for c in range(3):
                for part in range(2):
                    value = full[s][c][part]
                    if not first:
                        value = value + weave[part, s, c, cols, :]
                    weave[part, s, c, cols, :] = value

    def plane_group(index, carry):
        cols = group(index)
        psi = spinor(cols)
        upper = lower = None
        for mu in range(2):
            turned = small_times(singles[mu][:2, 2:], psi[2:])
            ahead = colour(mu, rolled_half(subtracted(psi[:2], turned), -1, mu == 1), False)
            behind = rolled_half(colour(mu, added(psi[:2], turned), True), 1, mu == 1)
            up = subtracted(ahead, behind)
            low = small_times(-singles[mu][2:, :2], added(ahead, behind))
            upper = up if upper is None else added(upper, up)
            lower = low if lower is None else added(lower, low)
        store_weave(cols, upper + lower, True)
        return carry

    lax.fori_loop(0, groups, plane_group, 0)

    for load in loads[3:]:
        load.wait()
    sites = lax.broadcasted_iota(jnp.int32, (8, plane), 1)
    coord_x = lax.rem(sites, width_x).astype(jnp.float32)
    coord_y = lax.div(sites, width_x).astype(jnp.float32)
    coord_z = here.astype(jnp.float32)
    phases = []
    for number in range(moments):
        momentum = [momenta_ref[number, axis].astype(jnp.float32) for axis in range(3)]
        turns = coord_x * (momentum[0] * (1.0 / width_x))
        turns = turns + coord_y * (momentum[1] * (width_x / plane))
        turns = turns + coord_z * (momentum[2] * (1.0 / full_z))
        theta = (2.0 * math.pi) * (turns - jnp.floor(turns))
        phases.append((jnp.cos(theta)[:1, :], jnp.sin(theta)[:1, :]))

    def arrange(owner, source):
        for part in range(2):
            for c in range(3):
                lane = (part * 3 + c) * plane
                for s in range(4):
                    for j in range(columns // rows):
                        row = (j * 4 + s) * rows
                        rows_scr[owner, row : row + rows, lane : lane + plane] = source[
                            part, s, c, j * rows : (j + 1) * rows, :
                        ]

    arrange(core, back_ref)

    @pl.when(core == 0)
    def _():
        pl.semaphore_wait(ready_sem, 1)
        back_copy.start()

    if relayed:
        @pl.when((here == 0) & (core == 0))
        def _():
            pl.semaphore_signal(near_sem, inc=1, device_id={"spin": 1 - core})

        @pl.when((here == 0) & (core == 1))
        def _():
            pl.semaphore_wait(near_sem, 1)
            for g in range(groups):
                halo_copy(g, 1).start()

    back_copy.wait_recv()
    arrange(1 - core, other_back)

    inner = (here != 0) & (here != last)
    far = jnp.where(2 * here < spaces, last, 0)

    def chunk_copy(g, number, step, relay=False):
        owner = lax.rem(here + step, spaces)
        source_ref = chunk_send.at[g, number, owner]
        if relay:
            source_ref = far_send.at[g, number]
            target = last - 1 if step == 1 else 1
            target_ref, recv_sem = relay_recv.at[g, number], relay_sems.at[g, number]
        else:
            target = owner
            target_ref, recv_sem = chunk_recv.at[number, g, step - 1], chunk_recv_sems.at[number]
        return pltpu.make_async_remote_copy(
            src_ref=source_ref,
            dst_ref=target_ref,
            send_sem=chunk_send_sem,
            recv_sem=recv_sem,
            device_id={"space": target},
        )

    def wait_all(ref, send_sem, recv_sem):
        copy = pltpu.make_async_remote_copy(
            src_ref=ref,
            dst_ref=ref,
            send_sem=send_sem,
            recv_sem=recv_sem,
            device_id={"space": after},
        )
        return copy

    def wait_chunks(number):
        def wait(first, end):
            ref = chunk_recv.at[number, :, first:end]
            wait_all(ref, chunk_send_sem, chunk_recv_sems.at[number]).wait_recv()

        if not relayed:
            wait(0, last)
            return
        pl.when(inner)(functools.partial(wait, 0, last))
        pl.when(here == 0)(functools.partial(wait, 1, last))
        pl.when(here == last)(functools.partial(wait, 0, last - 1))

    chunk_rows = 4 * rows
    order = sorted(range(1, spaces), key=lambda step: -min(step, spaces - step))
    def depth_group(g):
        wait_all(halo_recv.at[g], halo_send_sem, halo_recv_sems.at[g]).wait_recv()
        received = [
            [
                [
                    tuple(
                        halo_recv[g, side, part, spin, c].astype(jnp.float32)
                        for part in range(2)
                    )
                    for c in range(3)
                ]
                for spin in range(2)
            ]
            for side in range(2)
        ]
        ahead = colour(2, received[0], False)
        behind = received[1]
        upper = subtracted(ahead, behind)
        lower = small_times(-singles[2][2:, :2], added(ahead, behind))
        store_weave(group(g), upper + lower, False)

    def rotate(g, number, dot, top):
        cols = group(g)
        cosine, sine = phases[number]
        for s in range(4):
            for c in range(3):
                real = weave[0, s, c, cols, :]
                imag = weave[1, s, c, cols, :]
                turned_real = (cosine * real + sine * imag).astype(jnp.bfloat16)
                turned_imag = (cosine * imag - sine * real).astype(jnp.bfloat16)
                at = top + 2 * s * GROUP
                rows_at = slice(at, at + GROUP)
                rows_next = slice(at + GROUP, at + 2 * GROUP)
                lanes_at = slice(c * plane, (c + 1) * plane)
                lanes_next = slice((3 + c) * plane, (4 + c) * plane)
                weave_mm[dot, rows_at, lanes_at] = turned_real
                weave_mm[dot, rows_at, lanes_next] = turned_imag
                weave_mm[dot, rows_next, lanes_at] = turned_imag
                weave_mm[dot, rows_next, lanes_next] = -turned_real

    def send_far(g, number):
        pl.when(here == last)(chunk_copy(g, number, 1, True).start)
        pl.when(here == 0)(chunk_copy(g, number, last, True).start)

    def send_first(g, number):
        if not relayed:
            for step in order:
                chunk_copy(g, number, step).start()
            return
        for step in (1, last):
            pl.when(inner)(chunk_copy(g, number, step).start)

    def send_rest(those):
        for step in range(2, last):
            delayed = inner & (lax.rem(here + step, spaces) == far)
            for g in those:
                for number in range(moments):
                    pl.when(jnp.logical_not(delayed))(chunk_copy(g, number, step).start)
        for step in (1, last):
            near = here == (0 if step == 1 else last)
            for g in those:
                for number in range(moments):
                    pl.when(near)(chunk_copy(g, number, step).start)

    width = pair.shape[-1]

    def product(g, rows_in):
        return lax.dot_general(
            rows_in, weave_mm[g], (((1,), (1,)), ((), ())), preferred_element_type=jnp.float32
        )

    far_owner = lax.div(far * rows, columns)
    far_row = pl.multiple_of(lax.rem(far * 4 * rows, 4 * columns), chunk_rows)
    def far_product(g):
        value = product(g, rows_scr[far_owner, pl.ds(far_row, chunk_rows), :])
        for number in range(moments):
            piece = value[:, number * width : (number + 1) * width]
            far_send[g, number] = piece.astype(jnp.bfloat16)
            send_far(g, number)

    def full_product(g):
        value = product(g, rows_scr[...].reshape(8 * columns, 6 * plane))
        for number in range(moments):
            for owner in range(spaces):
                piece = value[
                    owner * chunk_rows : (owner + 1) * chunk_rows,
                    number * width : (number + 1) * width,
                ]
                pair[g, number, owner] = piece
                chunk_send[g, number, owner] = piece.astype(jnp.bfloat16)
            send_first(g, number)

    for g in range(groups):
        depth_group(g)
        for number in range(moments):
            rotate(g, number, g, number * width)
        if relayed:
            pl.when(jnp.logical_not(inner))(functools.partial(far_product, g))
            pl.when(inner)(functools.partial(full_product, g))
        else:
            full_product(g)
    if relayed:

        @pl.when(jnp.logical_not(inner))
        def _():
            for g in range(groups):
                full_product(g)
                if g < groups - 1:
                    pl.when(core == 1)(functools.partial(send_rest, range(g, g + 1)))

    if relayed:
        @pl.when((core == 1) & jnp.logical_not(inner))
        def _():
            pl.semaphore_wait(turn_sem, 1)
            send_rest(range(groups - 1, groups))

        @pl.when((core == 0) | inner)
        def _():
            send_rest(range(groups))

    if relayed:
        for g in range(groups):
            for number in range(moments):
                for step in range(2, last):

                    @pl.when(((here == 1) & (step == last - 1)) | ((here == last - 1) & (step == 2)))
                    def _(g=g, number=number, step=step):
                        chunk_copy(g, number, last, True).wait_recv()
                        target = lax.rem(here + step, spaces)
                        summed = pair[g, number, target] + relay_recv[g, number].astype(
                            jnp.float32
                        )
                        chunk_send[g, number, target] = summed.astype(jnp.bfloat16)
                        chunk_copy(g, number, step).start()

    def summed_piece(g, number):
        total = pair[g, number, here]
        for step in range(1, spaces):
            total = total + chunk_recv[number, g, step - 1].astype(jnp.float32)
        return total * scaling

    lane = lax.broadcasted_iota(jnp.int32, (rows, width), 1)
    slot = lax.div(lax.rem(lane, groups * GROUP), GROUP)
    back_copy.wait_send()
    wait_all(halo_send, halo_send_sem, halo_recv_sems.at[0]).wait_send()
    wait_all(chunk_send.at[:, :, :last], chunk_send_sem, chunk_recv_sems.at[0]).wait_send()
    if relayed:

        @pl.when((core == 0) & jnp.logical_not(inner))
        def _():
            pl.semaphore_signal(turn_sem, inc=1, device_id={"spin": 1 - core})

    for number in range(moments):
        if number == 0:
            wait_chunks(0)
        elif number == 1:
            for other in range(1, moments):
                wait_chunks(other)
        totals = [summed_piece(g, number) for g in range(groups)]
        parts = []
        for part in range(2):
            merged_rows = []
            for s in range(4):
                merged = None
                for g in range(groups):
                    value = totals[g][s * rows : (s + 1) * rows]
                    if g != part:
                        value = pltpu.roll(value, (width + (g - part) * GROUP) % width, 1)
                    merged = value if merged is None else jnp.where(slot == g, value, merged)
                merged_rows.append(merged)
            parts.append(merged_rows)
        for offset in range(4):
            sums = []
            for part in range(2):
                terms = []
                for s in range(4):
                    t = s ^ offset
                    value = parts[part][s]
                    terms.append(pltpu.roll(value, width - t * 2 * GROUP, 1) if t else value)
                sums.append(
                    {
                        (pair_at, sign): terms[pair_at] + terms[pair_at + 1]
                        if sign > 0
                        else terms[pair_at] - terms[pair_at + 1]
                        for pair_at in (0, 2)
                        for sign in (1, -1)
                    }
                )
            for index in range(len(basis)):
                if np.flatnonzero(basis[index][0])[0] != offset:
                    continue
                units = [complex(basis[index][s, s ^ offset]) for s in range(4)]
                for part in range(2):
                    source, signs = picked(units, part)
                    first = sums[source][0, signs[0] * signs[1]]
                    second = sums[source][2, signs[2] * signs[3]]
                    results[number, index, part] = signed_sum(signs[0], first, signs[2], second)
        for k in range(gammas):
            for part in range(2):
                out_ref[part, number, k] = results[number, gamma_ref[k], part][:, :columns]


def store_kernel(value_ref, out_hbm, sems):
    moments = value_ref.shape[1]
    stores = [
        pltpu.make_async_copy(
            value_ref.at[:, number], out_hbm.at[:, number], sems.at[number]
        )
        for number in range(moments)
    ]
    for store in stores:
        store.start()
    for store in stores:
        store.wait()


def body(mesh, backward, forward, gauge_links, momenta, gamma_list):
    spaces = mesh.shape["space"]
    _, times, _, columns, _, layers, plane = forward.shape
    moments = momenta.shape[0]
    gammas = gamma_list.shape[0]
    rows = columns * mesh.shape["spin"] // spaces
    groups = columns // GROUP
    back = jnp.transpose(backward, (0, 1, 2, 4, 5, 3, 6)).reshape(2, 4, 3, columns, plane)
    fwd = jnp.transpose(forward, (0, 1, 2, 4, 5, 3, 6)).reshape(2, 4, 3, columns, plane)
    link = jnp.transpose(gauge_links, (1, 2, 3, 4, 5, 0, 6)).reshape(3, 3, 3, 2, plane)
    full_z = layers * spaces
    scaling = 0.5 / math.sqrt(3.0 * plane * full_z)
    width = 8 * GROUP
    vmem = pl.BlockSpec(memory_space=pltpu.VMEM)
    anywhere = pl.BlockSpec(memory_space=pl.ANY)
    out_shape = (2, moments, gammas, rows, columns)
    values = pl.pallas_call(
        functools.partial(kernel, spaces, LX, full_z, scaling),
        out_shape=pltpu.VMEM(out_shape, jnp.float32),
        in_specs=[anywhere] * 5,
        out_specs=vmem,
        scratch_shapes=[
            pltpu.VMEM(back.shape, back.dtype),
            pltpu.VMEM(fwd.shape, fwd.dtype),
            pltpu.VMEM(link.shape, link.dtype),
            pltpu.SMEM(momenta.shape, momenta.dtype),
            pltpu.SMEM(gamma_list.shape, gamma_list.dtype),
            pltpu.VMEM((2, 4, 3, columns, plane), jnp.bfloat16),
            pltpu.VMEM((moments, 16, 2, rows, width), jnp.float32),
            pltpu.VMEM((56, plane), jnp.float32),
            pltpu.VMEM((groups, 2, 2, 2, 3, GROUP, plane), jnp.bfloat16),
            pltpu.VMEM((groups, 2, 2, 2, 3, GROUP, plane), jnp.bfloat16),
            pltpu.VMEM((2, 4 * columns, 6 * plane), jnp.bfloat16),
            pltpu.VMEM((2, 4, 3, columns, plane), jnp.float32),
            pltpu.VMEM((groups, moments * width, 6 * plane), jnp.bfloat16),
            pltpu.VMEM((groups, moments, spaces, 4 * rows, width), jnp.float32),
            pltpu.VMEM((groups, moments, spaces, 4 * rows, width), jnp.bfloat16),
            pltpu.VMEM((groups, moments, 4 * rows, width), jnp.bfloat16),
            pltpu.VMEM((moments, groups, spaces - 1, 4 * rows, width), jnp.bfloat16),
            pltpu.VMEM((groups, moments, 4 * rows, width), jnp.bfloat16),
            pltpu.SemaphoreType.DMA((5,)),
            pltpu.SemaphoreType.DMA((2,)),
            pltpu.SemaphoreType.DMA,
            pltpu.SemaphoreType.DMA((groups,)),
            pltpu.SemaphoreType.DMA,
            pltpu.SemaphoreType.DMA((moments,)),
            pltpu.SemaphoreType.DMA((groups, moments)),
            pltpu.SemaphoreType.REGULAR,
            pltpu.SemaphoreType.REGULAR,
            pltpu.SemaphoreType.REGULAR,
        ],
        compiler_params=pltpu.CompilerParams(collective_id=0, has_side_effects=True),
    )(back, fwd, link, momenta, gamma_list)
    out = pl.pallas_call(
        store_kernel,
        out_shape=jax.ShapeDtypeStruct(out_shape, jnp.float32),
        in_specs=[vmem],
        out_specs=anywhere,
        scratch_shapes=[pltpu.SemaphoreType.DMA((moments,))],
    )(pltpu.with_memory_space_constraint(values, pltpu.VMEM))
    return out.reshape(2, moments, gammas, times, rows, columns)


def solution(mesh):
    in_specs = (
        P("parts", "tm", None, "spin", None, "space", None),
        P("parts", "tm", None, "spin", None, "space", None),
        P("parts", None, None, None, "tm", "space", None),
        P(),
        P(),
    )
    out_specs = P("parts", None, None, "tm", "space", "spin")
    return jax.shard_map(
        functools.partial(body, mesh),
        mesh=mesh,
        in_specs=in_specs,
        out_specs=out_specs,
        check_vma=False,
    )
```

```python
import functools
import math

import jax
import jax.numpy as jnp
import numpy as np
from jax import lax
from jax.experimental import pallas as pl
from jax.experimental.pallas import tpu as pltpu
from jax.sharding import PartitionSpec as P

LX = 32
GROUP = 16
LINE = 4


def gamma_tables():
    zeros = np.zeros((4, 4))
    gx_imag = np.array([[0, 0, 0, 1], [0, 0, 1, 0], [0, -1, 0, 0], [-1, 0, 0, 0]]) * 1.0
    gy_real = np.array([[0, 0, 0, -1], [0, 0, 1, 0], [0, 1, 0, 0], [-1, 0, 0, 0]]) * 1.0
    gz_imag = np.array([[0, 0, 1, 0], [0, 0, 0, -1], [-1, 0, 0, 0], [0, 1, 0, 0]]) * 1.0
    gt_real = np.array([[0, 0, 1, 0], [0, 0, 0, 1], [1, 0, 0, 0], [0, 1, 0, 0]]) * 1.0
    singles = [zeros + 1j * gx_imag, gy_real + 0j, 1j * gz_imag, gt_real + 0j]
    basis = []
    for number in range(16):
        matrix = np.eye(4) + 0j
        for which in range(4):
            if number >> which & 1:
                matrix = matrix @ singles[which]
        basis.append(matrix)
    return singles, np.stack(basis)


def picked(units, part):
    if all(unit.imag == 0 for unit in units):
        return part, [int(unit.real) for unit in units]
    assert all(unit.real == 0 for unit in units)
    sign = -1 if part == 0 else 1
    return 1 - part, [sign * int(unit.imag) for unit in units]


def signed_sum(first_sign, first, second_sign, second):
    if first_sign > 0:
        return first + second if second_sign > 0 else first - second
    return second - first if second_sign > 0 else -first - second


def unit_times(unit, value):
    real, imag = value
    if unit == 1:
        return real, imag
    if unit == -1:
        return -real, -imag
    if unit == 1j:
        return -imag, real
    return imag, -real


def small_times(matrix, half):
    outs = []
    for row in range(2):
        column = int(np.flatnonzero(matrix[row])[0])
        outs.append([unit_times(complex(matrix[row, column]), value) for value in half[column]])
    return outs


def added(first, second):
    return [
        [(a[0] + b[0], a[1] + b[1]) for a, b in zip(left, right)]
        for left, right in zip(first, second)
    ]


def subtracted(first, second):
    return [
        [(a[0] - b[0], a[1] - b[1]) for a, b in zip(left, right)]
        for left, right in zip(first, second)
    ]


def kernel(
    spaces,
    width_x,
    full_z,
    scaling,
    back_hbm,
    fwd_hbm,
    link_hbm,
    momenta_hbm,
    gamma_hbm,
    out_ref,
    back_ref,
    fwd_ref,
    link_ref,
    momenta_ref,
    gamma_ref,
    other_back,
    results,
    links,
    halo_send,
    halo_recv,
    rows_scr,
    weave,
    weave_mm,
    pair,
    chunk_send,
    far_send,
    chunk_recv,
    relay_recv,
    load_sems,
    back_sems,
    halo_send_sem,
    halo_recv_sems,
    chunk_send_sem,
    chunk_recv_sems,
    relay_sems,
    ready_sem,
):
    loads = [
        pltpu.make_async_copy(source, target, load_sems.at[number])
        for number, (source, target) in enumerate(
            (
                (fwd_hbm, fwd_ref),
                (link_hbm, link_ref),
                (back_hbm, back_ref),
                (momenta_hbm, momenta_ref),
                (gamma_hbm, gamma_ref),
            )
        )
    ]
    for load in loads:
        load.start()
    columns = fwd_ref.shape[3]
    plane = fwd_ref.shape[4]
    moments = momenta_ref.shape[0]
    width = pair.shape[-1]
    gammas = gamma_ref.shape[0]
    groups = columns // GROUP
    rows = columns * 2 // spaces
    last = spaces - 1
    relayed = 4 <= spaces <= LINE
    here = lax.axis_index("space")
    core = lax.axis_index("spin")
    after = lax.rem(here + 1, spaces)
    before = lax.rem(here + last, spaces)
    singles, basis = gamma_tables()

    barrier = pltpu.get_barrier_semaphore()
    if relayed:
        greeted = 2
        for target in (before, after):
            pl.semaphore_signal(barrier, inc=1, device_id={"space": target})
    else:
        greeted = last
        for step in range(1, spaces):
            target = lax.rem(here + step, spaces)
            pl.semaphore_signal(barrier, inc=1, device_id={"space": target})

    @pl.when(core == 0)
    def _():
        pl.semaphore_signal(barrier, inc=1, device_id={"spin": 1 - core})

    if relayed:
        for g in range(groups):
            for number in range(moments):

                @pl.when(here == 0)
                def _(g=g, number=number):
                    chunk_recv[number, g, 0] = jnp.zeros_like(chunk_recv[number, g, 0])

                @pl.when(here == last)
                def _(g=g, number=number):
                    chunk_recv[number, g, last - 1] = jnp.zeros_like(chunk_recv[number, g, 0])

    for load in loads[:2]:
        load.wait()
    for mu in range(3):
        for c in range(3):
            for d in range(3):
                row = ((mu * 3 + c) * 3 + d) * 2
                links[row : row + 2, :] = link_ref[mu, c, d].astype(jnp.float32)

    def link(mu, c, d):
        row = ((mu * 3 + c) * 3 + d) * 2
        return [
            jnp.broadcast_to(links[row + part : row + part + 1, :], (GROUP, plane))
            for part in range(2)
        ]

    def colour(mu, half, dagger):
        outs = [[None] * 3 for _ in range(2)]
        for c in range(3):
            for d in range(3):
                u_real, u_imag = link(mu, d, c) if dagger else link(mu, c, d)
                for spin in range(2):
                    v_real, v_imag = half[spin][d]
                    if dagger:
                        real = u_real * v_real + u_imag * v_imag
                        imag = u_real * v_imag - u_imag * v_real
                    else:
                        real = u_real * v_real - u_imag * v_imag
                        imag = u_real * v_imag + u_imag * v_real
                    held = outs[spin][c]
                    outs[spin][c] = (
                        (real, imag) if held is None else (held[0] + real, held[1] + imag)
                    )
        return outs

    lanes = lax.broadcasted_iota(jnp.int32, (GROUP, plane), 1)
    column_x = lax.rem(lanes, width_x)

    def rolled(value, steps, along_y):
        if along_y:
            return pltpu.roll(value, (steps * width_x) % plane, 1)
        plain = pltpu.roll(value, steps % plane, 1)
        wrapped = pltpu.roll(value, (steps - steps * width_x) % plane, 1)
        edge = 0 if steps == 1 else width_x - 1
        return jnp.where(column_x == edge, wrapped, plain)

    def rolled_half(half, steps, along_y):
        return [
            [tuple(rolled(part, steps, along_y) for part in value) for value in spin]
            for spin in half
        ]

    def spinor(cols):
        return [
            [
                tuple(fwd_ref[part, s, c, cols, :].astype(jnp.float32) for part in range(2))
                for c in range(3)
            ]
            for s in range(4)
        ]

    def group(index):
        if isinstance(index, int):
            return slice(index * GROUP, (index + 1) * GROUP)
        return pl.ds(pl.multiple_of(index * GROUP, GROUP), GROUP)

    def halo_copy(g, side):
        return pltpu.make_async_remote_copy(
            src_ref=halo_send.at[g, side],
            dst_ref=halo_recv.at[g, side],
            send_sem=halo_send_sem,
            recv_sem=halo_recv_sems.at[g],
            device_id={"space": before if side == 0 else after},
        )

    for g in range(groups):
        psi = spinor(group(g))
        turned = small_times(singles[2][:2, 2:], psi[2:])
        minus = subtracted(psi[:2], turned)
        plus = colour(2, added(psi[:2], turned), True)
        for side, half in enumerate((minus, plus)):
            for spin in range(2):
                for c in range(3):
                    for part in range(2):
                        halo_send[g, side, part, spin, c] = half[spin][c][part].astype(
                            jnp.bfloat16
                        )
        if g == 0:
            pl.semaphore_wait(barrier, greeted + core)

        pl.when(here != last)(halo_copy(g, 0).start)
        pl.when(here != 0)(halo_copy(g, 1).start)
    for g in range(groups):
        pl.when(here == last)(halo_copy(g, 0).start)
        if relayed:
            pl.when((here == 0) & (core == 0))(halo_copy(g, 1).start)
        else:
            pl.when(here == 0)(halo_copy(g, 1).start)

    loads[2].wait()
    back_copy = pltpu.make_async_remote_copy(
        src_ref=back_ref,
        dst_ref=other_back,
        send_sem=back_sems.at[0],
        recv_sem=back_sems.at[1],
        device_id={"spin": 1 - core},
    )

    @pl.when(core == 1)
    def _():
        pl.semaphore_signal(ready_sem, inc=1, device_id={"spin": 1 - core})
        back_copy.start()

    def store_weave(cols, full):
        for s in range(4):
            for c in range(3):
                for part in range(2):
                    weave[part, s, c, cols, :] = full[s][c][part]

    def plane_group(index, carry):
        cols = group(index)
        psi = spinor(cols)
        upper = lower = None
        for mu in range(2):
            turned = small_times(singles[mu][:2, 2:], psi[2:])
            ahead = colour(mu, rolled_half(subtracted(psi[:2], turned), -1, mu == 1), False)
            behind = rolled_half(colour(mu, added(psi[:2], turned), True), 1, mu == 1)
            up = subtracted(ahead, behind)
            low = small_times(-singles[mu][2:, :2], added(ahead, behind))
            upper = up if upper is None else added(upper, up)
            lower = low if lower is None else added(lower, low)
        store_weave(cols, upper + lower)
        return carry

    lax.fori_loop(0, groups, plane_group, 0)

    for load in loads[3:]:
        load.wait()
    sites = lax.broadcasted_iota(jnp.int32, (8, plane), 1)
    coord_x = lax.rem(sites, width_x).astype(jnp.float32)
    coord_y = lax.div(sites, width_x).astype(jnp.float32)
    coord_z = here.astype(jnp.float32)
    phases = []
    for number in range(moments):
        momentum = [momenta_ref[number, axis].astype(jnp.float32) for axis in range(3)]
        turns = coord_x * (momentum[0] * (1.0 / width_x))
        turns = turns + coord_y * (momentum[1] * (width_x / plane))
        turns = turns + coord_z * (momentum[2] * (1.0 / full_z))
        theta = (2.0 * math.pi) * (turns - jnp.floor(turns))
        phases.append((jnp.cos(theta)[:1, :], jnp.sin(theta)[:1, :]))

    def arrange(owner, source):
        for part in range(2):
            for c in range(3):
                lane = (part * 3 + c) * plane
                for s in range(4):
                    for j in range(columns // rows):
                        row = (j * 4 + s) * rows
                        rows_scr[owner, row : row + rows, lane : lane + plane] = source[
                            part, s, c, j * rows : (j + 1) * rows, :
                        ]

    arrange(core, back_ref)

    @pl.when(core == 0)
    def _():
        pl.semaphore_wait(ready_sem, 1)
        back_copy.start()

    if relayed:
        @pl.when((here == 0) & (core == 0))
        def _():
            pl.semaphore_signal(ready_sem, inc=1, device_id={"spin": 1 - core})

        @pl.when((here == 0) & (core == 1))
        def _():
            pl.semaphore_wait(ready_sem, 1)
            for g in range(groups):
                halo_copy(g, 1).start()

    back_copy.wait_recv()
    arrange(1 - core, other_back)

    inner = (here != 0) & (here != last)
    far = jnp.where(2 * here < spaces, last, 0)

    def chunk_copy(g, number, step, relay=False):
        owner = lax.rem(here + step, spaces)
        source_ref = chunk_send.at[g, number, owner]
        if relay:
            source_ref = far_send.at[g, number]
            target = last - 1 if step == 1 else 1
            target_ref, recv_sem = relay_recv.at[g, number], relay_sems.at[g, number]
        else:
            target = owner
            target_ref, recv_sem = chunk_recv.at[number, g, step - 1], chunk_recv_sems.at[number]
        return pltpu.make_async_remote_copy(
            src_ref=source_ref,
            dst_ref=target_ref,
            send_sem=chunk_send_sem,
            recv_sem=recv_sem,
            device_id={"space": target},
        )

    def wait_all(ref, send_sem, recv_sem):
        copy = pltpu.make_async_remote_copy(
            src_ref=ref,
            dst_ref=ref,
            send_sem=send_sem,
            recv_sem=recv_sem,
            device_id={"space": after},
        )
        return copy

    def wait_chunks(number):
        def wait(first, end):
            ref = chunk_recv.at[number, :, first:end]
            wait_all(ref, chunk_send_sem, chunk_recv_sems.at[number]).wait_recv()

        if not relayed:
            wait(0, last)
            return
        pl.when(inner)(functools.partial(wait, 0, last))
        pl.when(here == 0)(functools.partial(wait, 1, last))
        pl.when(here == last)(functools.partial(wait, 0, last - 1))

    chunk_rows = 4 * rows
    order = sorted(range(1, spaces), key=lambda step: -min(step, spaces - step))
    def depth_group(g):
        wait_all(halo_recv.at[g], halo_send_sem, halo_recv_sems.at[g]).wait_recv()
        received = [
            [
                [
                    tuple(
                        halo_recv[g, side, part, spin, c].astype(jnp.float32)
                        for part in range(2)
                    )
                    for c in range(3)
                ]
                for spin in range(2)
            ]
            for side in range(2)
        ]
        ahead = colour(2, received[0], False)
        behind = received[1]
        upper = subtracted(ahead, behind)
        lower = small_times(-singles[2][2:, :2], added(ahead, behind))
        rotate(g, upper + lower)

    def rotate(g, full):
        cols = group(g)
        for s in range(4):
            for c in range(3):
                real, imag = full[s][c]
                real = real + weave[0, s, c, cols, :]
                imag = imag + weave[1, s, c, cols, :]
                lanes_at = slice(c * plane, (c + 1) * plane)
                lanes_next = slice((3 + c) * plane, (4 + c) * plane)
                for number in range(moments):
                    cosine, sine = phases[number]
                    turned_real = (cosine * real + sine * imag).astype(jnp.bfloat16)
                    turned_imag = (cosine * imag - sine * real).astype(jnp.bfloat16)
                    at = number * width + 2 * s * GROUP
                    rows_at = slice(at, at + GROUP)
                    rows_next = slice(at + GROUP, at + 2 * GROUP)
                    weave_mm[g, rows_at, lanes_at] = turned_real
                    weave_mm[g, rows_at, lanes_next] = turned_imag
                    weave_mm[g, rows_next, lanes_at] = turned_imag
                    weave_mm[g, rows_next, lanes_next] = -turned_real

    def send_far(g, number):
        pl.when(here == last)(chunk_copy(g, number, 1, True).start)
        pl.when(here == 0)(chunk_copy(g, number, last, True).start)

    def send_first(g, number):
        if not relayed:
            for step in order:
                chunk_copy(g, number, step).start()
            return
        for step in (1, last):
            pl.when(inner)(chunk_copy(g, number, step).start)

    def send_rest(those, phases_in=(0, 1)):
        for step in range(2, last):
            delayed = inner & (lax.rem(here + step, spaces) == far)
            for g in those:
                for number in range(moments):
                    if 0 in phases_in:
                        pl.when(jnp.logical_not(delayed))(chunk_copy(g, number, step).start)
        for step in (1, last):
            near = here == (0 if step == 1 else last)
            for g in those:
                for number in range(moments):
                    if 1 in phases_in:
                        pl.when(near)(chunk_copy(g, number, step).start)


    def product(g, rows_in):
        return lax.dot_general(
            rows_in, weave_mm[g], (((1,), (1,)), ((), ())), preferred_element_type=jnp.float32
        )

    far_owner = lax.div(far * rows, columns)
    far_row = pl.multiple_of(lax.rem(far * 4 * rows, 4 * columns), chunk_rows)
    def far_product(g):
        value = product(g, rows_scr[far_owner, pl.ds(far_row, chunk_rows), :])
        for number in range(moments):
            piece = value[:, number * width : (number + 1) * width]
            far_send[g, number] = piece.astype(jnp.bfloat16)
            send_far(g, number)

    def full_product(g):
        value = product(g, rows_scr[...].reshape(8 * columns, 6 * plane))
        for number in range(moments):
            for owner in range(spaces):
                piece = value[
                    owner * chunk_rows : (owner + 1) * chunk_rows,
                    number * width : (number + 1) * width,
                ]
                pair[g, number, owner] = piece
                chunk_send[g, number, owner] = piece.astype(jnp.bfloat16)
            send_first(g, number)

    for g in range(groups):
        depth_group(g)
        if relayed:
            pl.when(jnp.logical_not(inner))(functools.partial(far_product, g))
            pl.when(inner)(functools.partial(full_product, g))
        else:
            full_product(g)
    if relayed:

        @pl.when(jnp.logical_not(inner))
        def _():
            for g in range(groups):
                full_product(g)
                if g < groups - 1:
                    pl.when(core == 1)(functools.partial(send_rest, range(g, g + 1), (0,)))

    if relayed:
        @pl.when((core == 1) & jnp.logical_not(inner))
        def _():
            pl.semaphore_wait(ready_sem, 1)
            send_rest(range(groups - 1), (1,))
            send_rest(range(groups - 1, groups))

        @pl.when((core == 0) | inner)
        def _():
            send_rest(range(groups))

    if relayed:
        for g in range(groups):
            for number in range(moments):
                for step in range(2, last):

                    @pl.when(((here == 1) & (step == last - 1)) | ((here == last - 1) & (step == 2)))
                    def _(g=g, number=number, step=step):
                        chunk_copy(g, number, last, True).wait_recv()
                        target = lax.rem(here + step, spaces)
                        summed = pair[g, number, target] + relay_recv[g, number].astype(
                            jnp.float32
                        )
                        chunk_send[g, number, target] = summed.astype(jnp.bfloat16)
                        chunk_copy(g, number, step).start()

    def summed_piece(g, number):
        total = pair[g, number, here]
        for step in range(1, spaces):
            total = total + chunk_recv[number, g, step - 1].astype(jnp.float32)
        return total * scaling

    lane = lax.broadcasted_iota(jnp.int32, (rows, width), 1)
    slot = lax.div(lax.rem(lane, groups * GROUP), GROUP)
    back_copy.wait_send()
    wait_all(halo_send, halo_send_sem, halo_recv_sems.at[0]).wait_send()
    wait_all(chunk_send.at[:, :, :last], chunk_send_sem, chunk_recv_sems.at[0]).wait_send()
    if relayed:

        @pl.when((core == 0) & jnp.logical_not(inner))
        def _():
            pl.semaphore_signal(ready_sem, inc=1, device_id={"spin": 1 - core})

    for number in range(moments):
        if number == 0:
            wait_chunks(0)
        elif number == 1:
            for other in range(1, moments):
                wait_chunks(other)
        totals = [summed_piece(g, number) for g in range(groups)]
        parts = []
        for part in range(2):
            merged_rows = []
            for s in range(4):
                merged = None
                for g in range(groups):
                    value = totals[g][s * rows : (s + 1) * rows]
                    if g != part:
                        value = pltpu.roll(value, (width + (g - part) * GROUP) % width, 1)
                    merged = value if merged is None else jnp.where(slot == g, value, merged)
                merged_rows.append(merged)
            parts.append(merged_rows)
        for offset in range(4):
            sums = []
            for part in range(2):
                terms = []
                for s in range(4):
                    t = s ^ offset
                    value = parts[part][s]
                    terms.append(pltpu.roll(value, width - t * 2 * GROUP, 1) if t else value)
                sums.append(
                    {
                        (pair_at, sign): terms[pair_at] + terms[pair_at + 1]
                        if sign > 0
                        else terms[pair_at] - terms[pair_at + 1]
                        for pair_at in (0, 2)
                        for sign in (1, -1)
                    }
                )
            for index in range(len(basis)):
                if np.flatnonzero(basis[index][0])[0] != offset:
                    continue
                units = [complex(basis[index][s, s ^ offset]) for s in range(4)]
                for part in range(2):
                    source, signs = picked(units, part)
                    first = sums[source][0, signs[0] * signs[1]]
                    second = sums[source][2, signs[2] * signs[3]]
                    results[number, index, part] = signed_sum(signs[0], first, signs[2], second)
        for k in range(gammas):
            for part in range(2):
                out_ref[part, number, k] = results[number, gamma_ref[k], part][:, :columns]


def store_kernel(value_ref, out_hbm, sems):
    moments = value_ref.shape[1]
    stores = [
        pltpu.make_async_copy(
            value_ref.at[:, number], out_hbm.at[:, number], sems.at[number]
        )
        for number in range(moments)
    ]
    for store in stores:
        store.start()
    for store in stores:
        store.wait()


def body(mesh, backward, forward, gauge_links, momenta, gamma_list):
    spaces = mesh.shape["space"]
    _, times, _, columns, _, layers, plane = forward.shape
    moments = momenta.shape[0]
    gammas = gamma_list.shape[0]
    rows = columns * mesh.shape["spin"] // spaces
    groups = columns // GROUP
    back = jnp.transpose(backward, (0, 1, 2, 4, 5, 3, 6)).reshape(2, 4, 3, columns, plane)
    fwd = jnp.transpose(forward, (0, 1, 2, 4, 5, 3, 6)).reshape(2, 4, 3, columns, plane)
    link = jnp.transpose(gauge_links, (1, 2, 3, 4, 5, 0, 6)).reshape(3, 3, 3, 2, plane)
    full_z = layers * spaces
    scaling = 0.5 / math.sqrt(3.0 * plane * full_z)
    width = 8 * GROUP
    vmem = pl.BlockSpec(memory_space=pltpu.VMEM)
    anywhere = pl.BlockSpec(memory_space=pl.ANY)
    out_shape = (2, moments, gammas, rows, columns)
    values = pl.pallas_call(
        functools.partial(kernel, spaces, LX, full_z, scaling),
        out_shape=pltpu.VMEM(out_shape, jnp.float32),
        in_specs=[anywhere] * 5,
        out_specs=vmem,
        scratch_shapes=[
            pltpu.VMEM(back.shape, back.dtype),
            pltpu.VMEM(fwd.shape, fwd.dtype),
            pltpu.VMEM(link.shape, link.dtype),
            pltpu.SMEM(momenta.shape, momenta.dtype),
            pltpu.SMEM(gamma_list.shape, gamma_list.dtype),
            pltpu.VMEM((2, 4, 3, columns, plane), jnp.bfloat16),
            pltpu.VMEM((moments, 16, 2, rows, width), jnp.float32),
            pltpu.VMEM((56, plane), jnp.float32),
            pltpu.VMEM((groups, 2, 2, 2, 3, GROUP, plane), jnp.bfloat16),
            pltpu.VMEM((groups, 2, 2, 2, 3, GROUP, plane), jnp.bfloat16),
            pltpu.VMEM((2, 4 * columns, 6 * plane), jnp.bfloat16),
            pltpu.VMEM((2, 4, 3, columns, plane), jnp.float32),
            pltpu.VMEM((groups, moments * width, 6 * plane), jnp.bfloat16),
            pltpu.VMEM((groups, moments, spaces, 4 * rows, width), jnp.float32),
            pltpu.VMEM((groups, moments, spaces, 4 * rows, width), jnp.bfloat16),
            pltpu.VMEM((groups, moments, 4 * rows, width), jnp.bfloat16),
            pltpu.VMEM((moments, groups, spaces - 1, 4 * rows, width), jnp.bfloat16),
            pltpu.VMEM((groups, moments, 4 * rows, width), jnp.bfloat16),
            pltpu.SemaphoreType.DMA((5,)),
            pltpu.SemaphoreType.DMA((2,)),
            pltpu.SemaphoreType.DMA,
            pltpu.SemaphoreType.DMA((groups,)),
            pltpu.SemaphoreType.DMA,
            pltpu.SemaphoreType.DMA((moments,)),
            pltpu.SemaphoreType.DMA((groups, moments)),
            pltpu.SemaphoreType.REGULAR,
        ],
        compiler_params=pltpu.CompilerParams(collective_id=0, has_side_effects=True),
    )(back, fwd, link, momenta, gamma_list)
    out = pl.pallas_call(
        store_kernel,
        out_shape=jax.ShapeDtypeStruct(out_shape, jnp.float32),
        in_specs=[vmem],
        out_specs=anywhere,
        scratch_shapes=[pltpu.SemaphoreType.DMA((moments,))],
    )(pltpu.with_memory_space_constraint(values, pltpu.VMEM))
    return out.reshape(2, moments, gammas, times, rows, columns)


def solution(mesh):
    in_specs = (
        P("parts", "tm", None, "spin", None, "space", None),
        P("parts", "tm", None, "spin", None, "space", None),
        P("parts", None, None, None, "tm", "space", None),
        P(),
        P(),
    )
    out_specs = P("parts", None, None, "tm", "space", "spin")
    return jax.shard_map(
        functools.partial(body, mesh),
        mesh=mesh,
        in_specs=in_specs,
        out_specs=out_specs,
        check_vma=False,
    )
```

```python
import functools
import math

import jax
import jax.numpy as jnp
import numpy as np
from jax import lax
from jax.experimental import pallas as pl
from jax.experimental.pallas import tpu as pltpu
from jax.sharding import PartitionSpec as P

LX = 32
GROUP = 16
LINE = 4


def gamma_tables():
    zeros = np.zeros((4, 4))
    gx_imag = np.array([[0, 0, 0, 1], [0, 0, 1, 0], [0, -1, 0, 0], [-1, 0, 0, 0]]) * 1.0
    gy_real = np.array([[0, 0, 0, -1], [0, 0, 1, 0], [0, 1, 0, 0], [-1, 0, 0, 0]]) * 1.0
    gz_imag = np.array([[0, 0, 1, 0], [0, 0, 0, -1], [-1, 0, 0, 0], [0, 1, 0, 0]]) * 1.0
    gt_real = np.array([[0, 0, 1, 0], [0, 0, 0, 1], [1, 0, 0, 0], [0, 1, 0, 0]]) * 1.0
    singles = [zeros + 1j * gx_imag, gy_real + 0j, 1j * gz_imag, gt_real + 0j]
    basis = []
    for number in range(16):
        matrix = np.eye(4) + 0j
        for which in range(4):
            if number >> which & 1:
                matrix = matrix @ singles[which]
        basis.append(matrix)
    return singles, np.stack(basis)


def picked(units, part):
    if all(unit.imag == 0 for unit in units):
        return part, [int(unit.real) for unit in units]
    assert all(unit.real == 0 for unit in units)
    sign = -1 if part == 0 else 1
    return 1 - part, [sign * int(unit.imag) for unit in units]


def signed_sum(first_sign, first, second_sign, second):
    if first_sign > 0:
        return first + second if second_sign > 0 else first - second
    return second - first if second_sign > 0 else -first - second


def unit_times(unit, value):
    real, imag = value
    if unit == 1:
        return real, imag
    if unit == -1:
        return -real, -imag
    if unit == 1j:
        return -imag, real
    return imag, -real


def small_times(matrix, half):
    outs = []
    for row in range(2):
        column = int(np.flatnonzero(matrix[row])[0])
        outs.append([unit_times(complex(matrix[row, column]), value) for value in half[column]])
    return outs


def added(first, second):
    return [
        [(a[0] + b[0], a[1] + b[1]) for a, b in zip(left, right)]
        for left, right in zip(first, second)
    ]


def subtracted(first, second):
    return [
        [(a[0] - b[0], a[1] - b[1]) for a, b in zip(left, right)]
        for left, right in zip(first, second)
    ]


def kernel(
    spaces,
    width_x,
    full_z,
    scaling,
    back_hbm,
    fwd_hbm,
    link_hbm,
    momenta_hbm,
    gamma_hbm,
    out_ref,
    back_ref,
    fwd_ref,
    link_ref,
    momenta_ref,
    gamma_ref,
    other_back,
    results,
    links,
    halo_send,
    halo_recv,
    rows_scr,
    weave,
    weave_mm,
    pair,
    chunk_send,
    far_send,
    chunk_recv,
    relay_recv,
    load_sems,
    back_sems,
    halo_send_sem,
    halo_recv_sems,
    chunk_send_sem,
    chunk_recv_sems,
    relay_sems,
    ready_sem,
):
    loads = [
        pltpu.make_async_copy(source, target, load_sems.at[number])
        for number, (source, target) in enumerate(
            (
                (fwd_hbm, fwd_ref),
                (link_hbm, link_ref),
                (back_hbm, back_ref),
                (momenta_hbm, momenta_ref),
                (gamma_hbm, gamma_ref),
            )
        )
    ]
    for load in loads:
        load.start()
    columns = fwd_ref.shape[3]
    plane = fwd_ref.shape[4]
    moments = momenta_ref.shape[0]
    width = pair.shape[-1]
    gammas = gamma_ref.shape[0]
    groups = columns // GROUP
    rows = columns * 2 // spaces
    last = spaces - 1
    relayed = 4 <= spaces <= LINE
    here = lax.axis_index("space")
    core = lax.axis_index("spin")
    after = lax.rem(here + 1, spaces)
    before = lax.rem(here + last, spaces)
    singles, basis = gamma_tables()

    barrier = pltpu.get_barrier_semaphore()
    if relayed:
        greeted = 2
        for target in (before, after):
            pl.semaphore_signal(barrier, inc=1, device_id={"space": target})
    else:
        greeted = last
        for step in range(1, spaces):
            target = lax.rem(here + step, spaces)
            pl.semaphore_signal(barrier, inc=1, device_id={"space": target})

    @pl.when(core == 0)
    def _():
        pl.semaphore_signal(barrier, inc=1, device_id={"spin": 1 - core})

    if relayed:
        for g in range(groups):
            for number in range(moments):

                @pl.when((here == 0) & ((core == 1) if g == groups - 1 else (core >= 0)))
                def _(g=g, number=number):
                    chunk_recv[number, g * last] = jnp.zeros_like(chunk_recv[number, 0])

                @pl.when(here == last)
                def _(g=g, number=number):
                    chunk_recv[number, g * last + last - 1] = jnp.zeros_like(chunk_recv[number, 0])

    for load in loads[:2]:
        load.wait()
    for mu in range(3):
        for c in range(3):
            for d in range(3):
                row = ((mu * 3 + c) * 3 + d) * 2
                links[row : row + 2, :] = link_ref[mu, c, d].astype(jnp.float32)

    def link(mu, c, d):
        row = ((mu * 3 + c) * 3 + d) * 2
        return [
            jnp.broadcast_to(links[row + part : row + part + 1, :], (GROUP, plane))
            for part in range(2)
        ]

    def colour(mu, half, dagger):
        outs = [[None] * 3 for _ in range(2)]
        for c in range(3):
            for d in range(3):
                u_real, u_imag = link(mu, d, c) if dagger else link(mu, c, d)
                for spin in range(2):
                    v_real, v_imag = half[spin][d]
                    if dagger:
                        real = u_real * v_real + u_imag * v_imag
                        imag = u_real * v_imag - u_imag * v_real
                    else:
                        real = u_real * v_real - u_imag * v_imag
                        imag = u_real * v_imag + u_imag * v_real
                    held = outs[spin][c]
                    outs[spin][c] = (
                        (real, imag) if held is None else (held[0] + real, held[1] + imag)
                    )
        return outs

    lanes = lax.broadcasted_iota(jnp.int32, (GROUP, plane), 1)
    column_x = lax.rem(lanes, width_x)

    def rolled(value, steps, along_y):
        if along_y:
            return pltpu.roll(value, (steps * width_x) % plane, 1)
        plain = pltpu.roll(value, steps % plane, 1)
        wrapped = pltpu.roll(value, (steps - steps * width_x) % plane, 1)
        edge = 0 if steps == 1 else width_x - 1
        return jnp.where(column_x == edge, wrapped, plain)

    def rolled_half(half, steps, along_y):
        return [
            [tuple(rolled(part, steps, along_y) for part in value) for value in spin]
            for spin in half
        ]

    def spinor(cols):
        return [
            [
                tuple(fwd_ref[part, s, c, cols, :].astype(jnp.float32) for part in range(2))
                for c in range(3)
            ]
            for s in range(4)
        ]

    def group(index):
        if isinstance(index, int):
            return slice(index * GROUP, (index + 1) * GROUP)
        return pl.ds(pl.multiple_of(index * GROUP, GROUP), GROUP)

    def halo_copy(g, side):
        return pltpu.make_async_remote_copy(
            src_ref=halo_send.at[g, side],
            dst_ref=halo_recv.at[g, side],
            send_sem=halo_send_sem,
            recv_sem=halo_recv_sems.at[g],
            device_id={"space": before if side == 0 else after},
        )

    for g in range(groups):
        psi = spinor(group(g))
        turned = small_times(singles[2][:2, 2:], psi[2:])
        minus = subtracted(psi[:2], turned)
        plus = colour(2, added(psi[:2], turned), True)
        for side, half in enumerate((minus, plus)):
            for spin in range(2):
                for c in range(3):
                    for part in range(2):
                        halo_send[g, side, part, spin, c] = half[spin][c][part].astype(
                            jnp.bfloat16
                        )
        if g == 0:
            pl.semaphore_wait(barrier, greeted + core)

        pl.when(here != last)(halo_copy(g, 0).start)
        pl.when(here != 0)(halo_copy(g, 1).start)
    for g in range(groups):
        pl.when(here == last)(halo_copy(g, 0).start)
        if relayed:
            pl.when((here == 0) & (core == 0))(halo_copy(g, 1).start)
        else:
            pl.when(here == 0)(halo_copy(g, 1).start)

    loads[2].wait()
    back_copy = pltpu.make_async_remote_copy(
        src_ref=back_ref,
        dst_ref=other_back,
        send_sem=back_sems.at[0],
        recv_sem=back_sems.at[1],
        device_id={"spin": 1 - core},
    )

    @pl.when(core == 1)
    def _():
        pl.semaphore_signal(ready_sem, inc=1, device_id={"spin": 1 - core})
        back_copy.start()

    def store_weave(cols, full):
        for s in range(4):
            for c in range(3):
                for part in range(2):
                    weave[part, s, c, cols, :] = full[s][c][part]

    def plane_group(index, carry):
        cols = group(index)
        psi = spinor(cols)
        upper = lower = None
        for mu in range(2):
            turned = small_times(singles[mu][:2, 2:], psi[2:])
            ahead = colour(mu, rolled_half(subtracted(psi[:2], turned), -1, mu == 1), False)
            behind = rolled_half(colour(mu, added(psi[:2], turned), True), 1, mu == 1)
            up = subtracted(ahead, behind)
            low = small_times(-singles[mu][2:, :2], added(ahead, behind))
            upper = up if upper is None else added(upper, up)
            lower = low if lower is None else added(lower, low)
        store_weave(cols, upper + lower)
        return carry

    lax.fori_loop(0, groups, plane_group, 0)

    for load in loads[3:]:
        load.wait()
    sites = lax.broadcasted_iota(jnp.int32, (8, plane), 1)
    coord_x = lax.rem(sites, width_x).astype(jnp.float32)
    coord_y = lax.div(sites, width_x).astype(jnp.float32)
    coord_z = here.astype(jnp.float32)
    phases = []
    for number in range(moments):
        momentum = [momenta_ref[number, axis].astype(jnp.float32) for axis in range(3)]
        turns = coord_x * (momentum[0] * (1.0 / width_x))
        turns = turns + coord_y * (momentum[1] * (width_x / plane))
        turns = turns + coord_z * (momentum[2] * (1.0 / full_z))
        theta = (2.0 * math.pi) * (turns - jnp.floor(turns))
        phases.append((jnp.cos(theta)[:1, :], jnp.sin(theta)[:1, :]))

    def arrange(owner, source):
        for part in range(2):
            for c in range(3):
                lane = (part * 3 + c) * plane
                for s in range(4):
                    for j in range(columns // rows):
                        row = (j * 4 + s) * rows
                        rows_scr[owner, row : row + rows, lane : lane + plane] = source[
                            part, s, c, j * rows : (j + 1) * rows, :
                        ]

    arrange(core, back_ref)

    @pl.when(core == 0)
    def _():
        pl.semaphore_wait(ready_sem, 1)
        back_copy.start()

    if relayed:
        @pl.when((here == 0) & (core == 0))
        def _():
            pl.semaphore_signal(ready_sem, inc=1, device_id={"spin": 1 - core})

        @pl.when((here == 0) & (core == 1))
        def _():
            pl.semaphore_wait(ready_sem, 1)
            for g in range(groups):
                halo_copy(g, 1).start()

    back_copy.wait_recv()
    arrange(1 - core, other_back)

    inner = (here != 0) & (here != last)
    waiting = (here == last - 1) & (core == 0)
    far = jnp.where(2 * here < spaces, last, 0)

    def chunk_copy(g, number, step, relay=False):
        owner = lax.rem(here + step, spaces)
        source_ref = chunk_send.at[g, number, owner]
        if relay:
            source_ref = far_send.at[g, number]
            target = last - 1 if step == 1 else 1
            target_ref, recv_sem = relay_recv.at[g, number], relay_sems.at[g, number]
        else:
            target = owner
            target_ref, recv_sem = chunk_recv.at[number, g * last + step - 1], chunk_recv_sems.at[number]
        return pltpu.make_async_remote_copy(
            src_ref=source_ref,
            dst_ref=target_ref,
            send_sem=chunk_send_sem,
            recv_sem=recv_sem,
            device_id={"space": target},
        )

    def far_copy(g, number):
        return pltpu.make_async_remote_copy(
            src_ref=far_send.at[g, number],
            dst_ref=chunk_recv.at[number, g * last],
            send_sem=chunk_send_sem,
            recv_sem=chunk_recv_sems.at[number],
            device_id={"space": 0},
        )

    def wait_all(ref, send_sem, recv_sem):
        copy = pltpu.make_async_remote_copy(
            src_ref=ref,
            dst_ref=ref,
            send_sem=send_sem,
            recv_sem=recv_sem,
            device_id={"space": after},
        )
        return copy

    def wait_chunks(number):
        def wait(chunks):
            ref = chunk_recv.at[number, :chunks]
            wait_all(ref, chunk_send_sem, chunk_recv_sems.at[number]).wait_recv()

        if not relayed:
            wait(groups * last)
            return
        pl.when(inner)(functools.partial(wait, groups * last))
        pl.when((here == 0) & (core == 0))(functools.partial(wait, groups * last - groups + 1))
        pl.when((here == 0) & (core == 1))(functools.partial(wait, groups * last - groups))
        pl.when(here == last)(functools.partial(wait, groups * last - groups))

    chunk_rows = 4 * rows
    order = sorted(range(1, spaces), key=lambda step: -min(step, spaces - step))
    def depth_group(g):
        wait_all(halo_recv.at[g], halo_send_sem, halo_recv_sems.at[g]).wait_recv()
        received = [
            [
                [
                    tuple(
                        halo_recv[g, side, part, spin, c].astype(jnp.float32)
                        for part in range(2)
                    )
                    for c in range(3)
                ]
                for spin in range(2)
            ]
            for side in range(2)
        ]
        ahead = colour(2, received[0], False)
        behind = received[1]
        upper = subtracted(ahead, behind)
        lower = small_times(-singles[2][2:, :2], added(ahead, behind))
        rotate(g, upper + lower)

    def rotate(g, full):
        cols = group(g)
        for s in range(4):
            for c in range(3):
                real, imag = full[s][c]
                real = real + weave[0, s, c, cols, :]
                imag = imag + weave[1, s, c, cols, :]
                lanes_at = slice(c * plane, (c + 1) * plane)
                lanes_next = slice((3 + c) * plane, (4 + c) * plane)
                for number in range(moments):
                    cosine, sine = phases[number]
                    turned_real = (cosine * real + sine * imag).astype(jnp.bfloat16)
                    turned_imag = (cosine * imag - sine * real).astype(jnp.bfloat16)
                    at = number * width + 2 * s * GROUP
                    rows_at = slice(at, at + GROUP)
                    rows_next = slice(at + GROUP, at + 2 * GROUP)
                    weave_mm[g, rows_at, lanes_at] = turned_real
                    weave_mm[g, rows_at, lanes_next] = turned_imag
                    weave_mm[g, rows_next, lanes_at] = turned_imag
                    weave_mm[g, rows_next, lanes_next] = -turned_real

    def send_far(g, number):
        pl.when(here == 0)(chunk_copy(g, number, last, True).start)
        if g < groups - 1:
            pl.when(here == last)(chunk_copy(g, number, 1, True).start)
        else:
            pl.when((here == last) & (core == 1))(chunk_copy(g, number, 1, True).start)
            pl.when((here == last) & (core == 0))(far_copy(g, number).start)

    def send_first(g, number):
        if not relayed:
            for step in order:
                chunk_copy(g, number, step).start()
            return
        pl.when(inner)(chunk_copy(g, number, 1).start)
        pl.when(inner & jnp.logical_not(waiting))(chunk_copy(g, number, last).start)
        if g == groups - 1:
            pl.when(waiting)(chunk_copy(g, number, 2).start)

    def send_rest(those, phases_in=(0, 1)):
        for step in range(2, last):
            delayed = inner & (lax.rem(here + step, spaces) == far)
            for g in those:
                for number in range(moments):
                    if 0 in phases_in:
                        pl.when(jnp.logical_not(delayed))(chunk_copy(g, number, step).start)
        for step in (1, last):
            near = here == (0 if step == 1 else last)
            for g in those:
                for number in range(moments):
                    if 1 in phases_in:
                        pl.when(near)(chunk_copy(g, number, step).start)


    def product(g, rows_in):
        return lax.dot_general(
            rows_in, weave_mm[g], (((1,), (1,)), ((), ())), preferred_element_type=jnp.float32
        )

    far_owner = lax.div(far * rows, columns)
    far_row = pl.multiple_of(lax.rem(far * 4 * rows, 4 * columns), chunk_rows)
    def far_product(g):
        value = product(g, rows_scr[far_owner, pl.ds(far_row, chunk_rows), :])
        for number in range(moments):
            piece = value[:, number * width : (number + 1) * width]
            far_send[g, number] = piece.astype(jnp.bfloat16)
            send_far(g, number)

    def full_product(g):
        value = product(g, rows_scr[...].reshape(8 * columns, 6 * plane))
        for number in range(moments):
            for owner in range(spaces):
                piece = value[
                    owner * chunk_rows : (owner + 1) * chunk_rows,
                    number * width : (number + 1) * width,
                ]
                pair[g, number, owner] = piece
                chunk_send[g, number, owner] = piece.astype(jnp.bfloat16)
            send_first(g, number)

    for g in range(groups):
        depth_group(g)
        if relayed:
            pl.when(jnp.logical_not(inner))(functools.partial(far_product, g))
            pl.when(inner)(functools.partial(full_product, g))
        else:
            full_product(g)
    if relayed:

        @pl.when(jnp.logical_not(inner))
        def _():
            for g in range(groups):
                full_product(g)
                if g < groups - 1:
                    pl.when(core == 1)(functools.partial(send_rest, range(g, g + 1), (0,)))

    if relayed:
        @pl.when((core == 1) & jnp.logical_not(inner))
        def _():
            pl.semaphore_wait(ready_sem, 1)
            send_rest(range(groups - 1), (1,))
            send_rest(range(groups - 1, groups))

        @pl.when((core == 0) | inner)
        def _():
            send_rest(range(groups))

    if relayed:
        for g in range(groups):
            for number in range(moments):
                for step in range(2, last):

                    @pl.when(((here == 1) & (step == last - 1)) | ((here == last - 1) & (step == 2) & ((core == 1) if g == groups - 1 else (core >= 0))))
                    def _(g=g, number=number, step=step):
                        chunk_copy(g, number, last, True).wait_recv()
                        target = lax.rem(here + step, spaces)
                        summed = pair[g, number, target] + relay_recv[g, number].astype(
                            jnp.float32
                        )
                        chunk_send[g, number, target] = summed.astype(jnp.bfloat16)
                        chunk_copy(g, number, step).start()

    def summed_piece(g, number):
        total = pair[g, number, here]
        for step in range(1, spaces):
            total = total + chunk_recv[number, g * last + step - 1].astype(jnp.float32)
        return total * scaling

    if relayed:

        @pl.when(waiting)
        def _():
            for g in range(groups):
                for number in range(moments):
                    chunk_copy(g, number, last).start()

    lane = lax.broadcasted_iota(jnp.int32, (rows, width), 1)
    slot = lax.div(lax.rem(lane, groups * GROUP), GROUP)
    back_copy.wait_send()
    wait_all(halo_send, halo_send_sem, halo_recv_sems.at[0]).wait_send()
    wait_all(chunk_send.at[:, :, :last], chunk_send_sem, chunk_recv_sems.at[0]).wait_send()
    if relayed:

        @pl.when((core == 0) & jnp.logical_not(inner))
        def _():
            pl.semaphore_signal(ready_sem, inc=1, device_id={"spin": 1 - core})

    for number in range(moments):
        if number == 0:
            wait_chunks(0)
        elif number == 1:
            for other in range(1, moments):
                wait_chunks(other)
        totals = [summed_piece(g, number) for g in range(groups)]
        parts = []
        for part in range(2):
            merged_rows = []
            for s in range(4):
                merged = None
                for g in range(groups):
                    value = totals[g][s * rows : (s + 1) * rows]
                    if g != part:
                        value = pltpu.roll(value, (width + (g - part) * GROUP) % width, 1)
                    merged = value if merged is None else jnp.where(slot == g, value, merged)
                merged_rows.append(merged)
            parts.append(merged_rows)
        for offset in range(4):
            sums = []
            for part in range(2):
                terms = []
                for s in range(4):
                    t = s ^ offset
                    value = parts[part][s]
                    terms.append(pltpu.roll(value, width - t * 2 * GROUP, 1) if t else value)
                sums.append(
                    {
                        (pair_at, sign): terms[pair_at] + terms[pair_at + 1]
                        if sign > 0
                        else terms[pair_at] - terms[pair_at + 1]
                        for pair_at in (0, 2)
                        for sign in (1, -1)
                    }
                )
            for index in range(len(basis)):
                if np.flatnonzero(basis[index][0])[0] != offset:
                    continue
                units = [complex(basis[index][s, s ^ offset]) for s in range(4)]
                for part in range(2):
                    source, signs = picked(units, part)
                    first = sums[source][0, signs[0] * signs[1]]
                    second = sums[source][2, signs[2] * signs[3]]
                    results[number, index, part] = signed_sum(signs[0], first, signs[2], second)
        for k in range(gammas):
            for part in range(2):
                out_ref[part, number, k] = results[number, gamma_ref[k], part][:, :columns]


def store_kernel(value_ref, out_hbm, sems):
    moments = value_ref.shape[1]
    stores = [
        pltpu.make_async_copy(
            value_ref.at[:, number], out_hbm.at[:, number], sems.at[number]
        )
        for number in range(moments)
    ]
    for store in stores:
        store.start()
    for store in stores:
        store.wait()


def body(mesh, backward, forward, gauge_links, momenta, gamma_list):
    spaces = mesh.shape["space"]
    _, times, _, columns, _, layers, plane = forward.shape
    moments = momenta.shape[0]
    gammas = gamma_list.shape[0]
    rows = columns * mesh.shape["spin"] // spaces
    groups = columns // GROUP
    back = jnp.transpose(backward, (0, 1, 2, 4, 5, 3, 6)).reshape(2, 4, 3, columns, plane)
    fwd = jnp.transpose(forward, (0, 1, 2, 4, 5, 3, 6)).reshape(2, 4, 3, columns, plane)
    link = jnp.transpose(gauge_links, (1, 2, 3, 4, 5, 0, 6)).reshape(3, 3, 3, 2, plane)
    full_z = layers * spaces
    scaling = 0.5 / math.sqrt(3.0 * plane * full_z)
    width = 8 * GROUP
    vmem = pl.BlockSpec(memory_space=pltpu.VMEM)
    anywhere = pl.BlockSpec(memory_space=pl.ANY)
    out_shape = (2, moments, gammas, rows, columns)
    values = pl.pallas_call(
        functools.partial(kernel, spaces, LX, full_z, scaling),
        out_shape=pltpu.VMEM(out_shape, jnp.float32),
        in_specs=[anywhere] * 5,
        out_specs=vmem,
        scratch_shapes=[
            pltpu.VMEM(back.shape, back.dtype),
            pltpu.VMEM(fwd.shape, fwd.dtype),
            pltpu.VMEM(link.shape, link.dtype),
            pltpu.SMEM(momenta.shape, momenta.dtype),
            pltpu.SMEM(gamma_list.shape, gamma_list.dtype),
            pltpu.VMEM((2, 4, 3, columns, plane), jnp.bfloat16),
            pltpu.VMEM((moments, 16, 2, rows, width), jnp.float32),
            pltpu.VMEM((56, plane), jnp.float32),
            pltpu.VMEM((groups, 2, 2, 2, 3, GROUP, plane), jnp.bfloat16),
            pltpu.VMEM((groups, 2, 2, 2, 3, GROUP, plane), jnp.bfloat16),
            pltpu.VMEM((2, 4 * columns, 6 * plane), jnp.bfloat16),
            pltpu.VMEM((2, 4, 3, columns, plane), jnp.float32),
            pltpu.VMEM((groups, moments * width, 6 * plane), jnp.bfloat16),
            pltpu.VMEM((groups, moments, spaces, 4 * rows, width), jnp.float32),
            pltpu.VMEM((groups, moments, spaces, 4 * rows, width), jnp.bfloat16),
            pltpu.VMEM((groups, moments, 4 * rows, width), jnp.bfloat16),
            pltpu.VMEM((moments, groups * (spaces - 1), 4 * rows, width), jnp.bfloat16),
            pltpu.VMEM((groups, moments, 4 * rows, width), jnp.bfloat16),
            pltpu.SemaphoreType.DMA((5,)),
            pltpu.SemaphoreType.DMA((2,)),
            pltpu.SemaphoreType.DMA,
            pltpu.SemaphoreType.DMA((groups,)),
            pltpu.SemaphoreType.DMA,
            pltpu.SemaphoreType.DMA((moments,)),
            pltpu.SemaphoreType.DMA((groups, moments)),
            pltpu.SemaphoreType.REGULAR,
        ],
        compiler_params=pltpu.CompilerParams(collective_id=0, has_side_effects=True),
    )(back, fwd, link, momenta, gamma_list)
    out = pl.pallas_call(
        store_kernel,
        out_shape=jax.ShapeDtypeStruct(out_shape, jnp.float32),
        in_specs=[vmem],
        out_specs=anywhere,
        scratch_shapes=[pltpu.SemaphoreType.DMA((moments,))],
    )(pltpu.with_memory_space_constraint(values, pltpu.VMEM))
    return out.reshape(2, moments, gammas, times, rows, columns)


def solution(mesh):
    in_specs = (
        P("parts", "tm", None, "spin", None, "space", None),
        P("parts", "tm", None, "spin", None, "space", None),
        P("parts", None, None, None, "tm", "space", None),
        P(),
        P(),
    )
    out_specs = P("parts", None, None, "tm", "space", "spin")
    return jax.shard_map(
        functools.partial(body, mesh),
        mesh=mesh,
        in_specs=in_specs,
        out_specs=out_specs,
        check_vma=False,
    )
```

```python
import functools
import math

import jax
import jax.numpy as jnp
import numpy as np
from jax import lax
from jax.experimental import pallas as pl
from jax.experimental.pallas import tpu as pltpu
from jax.sharding import PartitionSpec as P

LX = 32
GROUP = 16
LINE = 4


def gamma_tables():
    zeros = np.zeros((4, 4))
    gx_imag = np.array([[0, 0, 0, 1], [0, 0, 1, 0], [0, -1, 0, 0], [-1, 0, 0, 0]]) * 1.0
    gy_real = np.array([[0, 0, 0, -1], [0, 0, 1, 0], [0, 1, 0, 0], [-1, 0, 0, 0]]) * 1.0
    gz_imag = np.array([[0, 0, 1, 0], [0, 0, 0, -1], [-1, 0, 0, 0], [0, 1, 0, 0]]) * 1.0
    gt_real = np.array([[0, 0, 1, 0], [0, 0, 0, 1], [1, 0, 0, 0], [0, 1, 0, 0]]) * 1.0
    singles = [zeros + 1j * gx_imag, gy_real + 0j, 1j * gz_imag, gt_real + 0j]
    basis = []
    for number in range(16):
        matrix = np.eye(4) + 0j
        for which in range(4):
            if number >> which & 1:
                matrix = matrix @ singles[which]
        basis.append(matrix)
    return singles, np.stack(basis)


def picked(units, part):
    if all(unit.imag == 0 for unit in units):
        return part, [int(unit.real) for unit in units]
    assert all(unit.real == 0 for unit in units)
    sign = -1 if part == 0 else 1
    return 1 - part, [sign * int(unit.imag) for unit in units]


def signed_sum(first_sign, first, second_sign, second):
    if first_sign > 0:
        return first + second if second_sign > 0 else first - second
    return second - first if second_sign > 0 else -first - second


def unit_times(unit, value):
    real, imag = value
    if unit == 1:
        return real, imag
    if unit == -1:
        return -real, -imag
    if unit == 1j:
        return -imag, real
    return imag, -real


def small_times(matrix, half):
    outs = []
    for row in range(2):
        column = int(np.flatnonzero(matrix[row])[0])
        outs.append([unit_times(complex(matrix[row, column]), value) for value in half[column]])
    return outs


def added(first, second):
    return [
        [(a[0] + b[0], a[1] + b[1]) for a, b in zip(left, right)]
        for left, right in zip(first, second)
    ]


def subtracted(first, second):
    return [
        [(a[0] - b[0], a[1] - b[1]) for a, b in zip(left, right)]
        for left, right in zip(first, second)
    ]


def kernel(
    spaces,
    width_x,
    full_z,
    scaling,
    back_hbm,
    fwd_hbm,
    link_hbm,
    momenta_hbm,
    gamma_hbm,
    out_ref,
    back_ref,
    fwd_ref,
    link_ref,
    momenta_ref,
    gamma_ref,
    other_back,
    results,
    links,
    halo_send,
    halo_recv,
    rows_scr,
    weave,
    weave_mm,
    pair,
    chunk_send,
    far_send,
    chunk_recv,
    relay_recv,
    load_sems,
    back_sems,
    halo_send_sem,
    halo_recv_sems,
    chunk_send_sem,
    chunk_recv_sems,
    relay_sems,
    ready_sem,
):
    loads = [
        pltpu.make_async_copy(source, target, load_sems.at[number])
        for number, (source, target) in enumerate(
            (
                (fwd_hbm, fwd_ref),
                (link_hbm, link_ref),
                (back_hbm, back_ref),
                (momenta_hbm, momenta_ref),
                (gamma_hbm, gamma_ref),
            )
        )
    ]
    for load in loads:
        load.start()
    columns = fwd_ref.shape[3]
    plane = fwd_ref.shape[4]
    moments = momenta_ref.shape[0]
    width = pair.shape[-1]
    gammas = gamma_ref.shape[0]
    groups = columns // GROUP
    rows = columns * 2 // spaces
    last = spaces - 1
    relayed = 4 <= spaces <= LINE
    here = lax.axis_index("space")
    core = lax.axis_index("spin")
    after = lax.rem(here + 1, spaces)
    before = lax.rem(here + last, spaces)
    singles, basis = gamma_tables()

    barrier = pltpu.get_barrier_semaphore()
    if relayed:
        greeted = 2
        for target in (before, after):
            pl.semaphore_signal(barrier, inc=1, device_id={"space": target})
    else:
        greeted = last
        for step in range(1, spaces):
            target = lax.rem(here + step, spaces)
            pl.semaphore_signal(barrier, inc=1, device_id={"space": target})

    @pl.when(core == 0)
    def _():
        pl.semaphore_signal(barrier, inc=1, device_id={"spin": 1 - core})

    if relayed:
        for g in range(groups):
            for number in range(moments):

                @pl.when((here == 0) & ((core == 1) if g == groups - 1 else (core >= 0)))
                def _(g=g, number=number):
                    chunk_recv[number, g * last] = jnp.zeros_like(chunk_recv[number, 0])

                @pl.when(here == last)
                def _(g=g, number=number):
                    chunk_recv[number, g * last + last - 1] = jnp.zeros_like(chunk_recv[number, 0])

    for load in loads[:2]:
        load.wait()
    for mu in range(3):
        for c in range(3):
            for d in range(3):
                row = ((mu * 3 + c) * 3 + d) * 2
                links[row : row + 2, :] = link_ref[mu, c, d].astype(jnp.float32)

    def link(mu, c, d):
        row = ((mu * 3 + c) * 3 + d) * 2
        return [
            jnp.broadcast_to(links[row + part : row + part + 1, :], (GROUP, plane))
            for part in range(2)
        ]

    def colour(mu, half, dagger):
        outs = [[None] * 3 for _ in range(2)]
        for c in range(3):
            for d in range(3):
                u_real, u_imag = link(mu, d, c) if dagger else link(mu, c, d)
                for spin in range(2):
                    v_real, v_imag = half[spin][d]
                    if dagger:
                        real = u_real * v_real + u_imag * v_imag
                        imag = u_real * v_imag - u_imag * v_real
                    else:
                        real = u_real * v_real - u_imag * v_imag
                        imag = u_real * v_imag + u_imag * v_real
                    held = outs[spin][c]
                    outs[spin][c] = (
                        (real, imag) if held is None else (held[0] + real, held[1] + imag)
                    )
        return outs

    lanes = lax.broadcasted_iota(jnp.int32, (GROUP, plane), 1)
    column_x = lax.rem(lanes, width_x)

    def rolled(value, steps, along_y):
        if along_y:
            return pltpu.roll(value, (steps * width_x) % plane, 1)
        plain = pltpu.roll(value, steps % plane, 1)
        wrapped = pltpu.roll(value, (steps - steps * width_x) % plane, 1)
        edge = 0 if steps == 1 else width_x - 1
        return jnp.where(column_x == edge, wrapped, plain)

    def rolled_half(half, steps, along_y):
        return [
            [tuple(rolled(part, steps, along_y) for part in value) for value in spin]
            for spin in half
        ]

    def spinor(cols):
        return [
            [
                tuple(fwd_ref[part, s, c, cols, :].astype(jnp.float32) for part in range(2))
                for c in range(3)
            ]
            for s in range(4)
        ]

    def group(index):
        if isinstance(index, int):
            return slice(index * GROUP, (index + 1) * GROUP)
        return pl.ds(pl.multiple_of(index * GROUP, GROUP), GROUP)

    def halo_copy(g, side):
        return pltpu.make_async_remote_copy(
            src_ref=halo_send.at[g, side],
            dst_ref=halo_recv.at[g, side],
            send_sem=halo_send_sem,
            recv_sem=halo_recv_sems.at[g],
            device_id={"space": before if side == 0 else after},
        )

    for g in range(groups):
        psi = spinor(group(g))
        turned = small_times(singles[2][:2, 2:], psi[2:])
        minus = subtracted(psi[:2], turned)
        plus = colour(2, added(psi[:2], turned), True)
        for side, half in enumerate((minus, plus)):
            for spin in range(2):
                for c in range(3):
                    for part in range(2):
                        halo_send[g, side, part, spin, c] = half[spin][c][part].astype(
                            jnp.bfloat16
                        )
        if g == 0:
            pl.semaphore_wait(barrier, greeted + core)

        pl.when(here != last)(halo_copy(g, 0).start)
        pl.when(here != 0)(halo_copy(g, 1).start)
    for g in range(groups):
        pl.when(here == last)(halo_copy(g, 0).start)
        if relayed:
            pl.when((here == 0) & (core == 0))(halo_copy(g, 1).start)
        else:
            pl.when(here == 0)(halo_copy(g, 1).start)

    loads[2].wait()
    back_copy = pltpu.make_async_remote_copy(
        src_ref=back_ref,
        dst_ref=other_back,
        send_sem=back_sems.at[0],
        recv_sem=back_sems.at[1],
        device_id={"spin": 1 - core},
    )

    @pl.when(core == 1)
    def _():
        pl.semaphore_signal(ready_sem, inc=1, device_id={"spin": 1 - core})
        back_copy.start()

    def store_weave(cols, full):
        for s in range(4):
            for c in range(3):
                for part in range(2):
                    weave[part, s, c, cols, :] = full[s][c][part]

    def plane_group(index, carry):
        cols = group(index)
        psi = spinor(cols)
        upper = lower = None
        for mu in range(2):
            turned = small_times(singles[mu][:2, 2:], psi[2:])
            ahead = colour(mu, rolled_half(subtracted(psi[:2], turned), -1, mu == 1), False)
            behind = rolled_half(colour(mu, added(psi[:2], turned), True), 1, mu == 1)
            up = subtracted(ahead, behind)
            low = small_times(-singles[mu][2:, :2], added(ahead, behind))
            upper = up if upper is None else added(upper, up)
            lower = low if lower is None else added(lower, low)
        store_weave(cols, upper + lower)
        return carry

    lax.fori_loop(0, groups, plane_group, 0)

    for load in loads[3:]:
        load.wait()
    sites = lax.broadcasted_iota(jnp.int32, (8, plane), 1)
    coord_x = lax.rem(sites, width_x).astype(jnp.float32)
    coord_y = lax.div(sites, width_x).astype(jnp.float32)
    coord_z = here.astype(jnp.float32)
    phases = []
    for number in range(moments):
        momentum = [momenta_ref[number, axis].astype(jnp.float32) for axis in range(3)]
        turns = coord_x * (momentum[0] * (1.0 / width_x))
        turns = turns + coord_y * (momentum[1] * (width_x / plane))
        turns = turns + coord_z * (momentum[2] * (1.0 / full_z))
        theta = (2.0 * math.pi) * (turns - jnp.floor(turns))
        phases.append((jnp.cos(theta)[:1, :], jnp.sin(theta)[:1, :]))

    def arrange(owner, source):
        for part in range(2):
            for c in range(3):
                lane = (part * 3 + c) * plane
                for s in range(4):
                    for j in range(columns // rows):
                        row = (j * 4 + s) * rows
                        rows_scr[owner, row : row + rows, lane : lane + plane] = source[
                            part, s, c, j * rows : (j + 1) * rows, :
                        ]

    arrange(core, back_ref)

    @pl.when(core == 0)
    def _():
        pl.semaphore_wait(ready_sem, 1)
        back_copy.start()

    if relayed:
        @pl.when((here == 0) & (core == 0))
        def _():
            pl.semaphore_signal(ready_sem, inc=1, device_id={"spin": 1 - core})

        @pl.when((here == 0) & (core == 1))
        def _():
            pl.semaphore_wait(ready_sem, 1)
            for g in range(groups):
                halo_copy(g, 1).start()

    back_copy.wait_recv()
    arrange(1 - core, other_back)

    inner = (here != 0) & (here != last)
    waiting = (here == last - 1) & (core == 0)
    far = jnp.where(2 * here < spaces, last, 0)

    def chunk_copy(g, number, step, relay=False):
        owner = lax.rem(here + step, spaces)
        source_ref = chunk_send.at[g, number, owner]
        if relay:
            source_ref = far_send.at[g, number]
            target = last - 1 if step == 1 else 1
            target_ref, recv_sem = relay_recv.at[g, number], relay_sems.at[g, number]
        else:
            target = owner
            target_ref, recv_sem = chunk_recv.at[number, g * last + step - 1], chunk_recv_sems.at[number]
        return pltpu.make_async_remote_copy(
            src_ref=source_ref,
            dst_ref=target_ref,
            send_sem=chunk_send_sem,
            recv_sem=recv_sem,
            device_id={"space": target},
        )

    def far_copy(g, number):
        return pltpu.make_async_remote_copy(
            src_ref=far_send.at[g, number],
            dst_ref=chunk_recv.at[number, g * last],
            send_sem=chunk_send_sem,
            recv_sem=chunk_recv_sems.at[number],
            device_id={"space": 0},
        )

    def wait_all(ref, send_sem, recv_sem):
        copy = pltpu.make_async_remote_copy(
            src_ref=ref,
            dst_ref=ref,
            send_sem=send_sem,
            recv_sem=recv_sem,
            device_id={"space": after},
        )
        return copy

    def wait_chunks(number):
        def wait(chunks):
            ref = chunk_recv.at[number, :chunks]
            wait_all(ref, chunk_send_sem, chunk_recv_sems.at[number]).wait_recv()

        if not relayed:
            wait(groups * last)
            return
        pl.when(inner)(functools.partial(wait, groups * last))
        pl.when((here == 0) & (core == 0))(functools.partial(wait, groups * last - groups + 1))
        pl.when((here == 0) & (core == 1))(functools.partial(wait, groups * last - groups))
        pl.when(here == last)(functools.partial(wait, groups * last - groups))

    chunk_rows = 4 * rows
    order = sorted(range(1, spaces), key=lambda step: -min(step, spaces - step))
    def depth_group(g):
        wait_all(halo_recv.at[g], halo_send_sem, halo_recv_sems.at[g]).wait_recv()
        received = [
            [
                [
                    tuple(
                        halo_recv[g, side, part, spin, c].astype(jnp.float32)
                        for part in range(2)
                    )
                    for c in range(3)
                ]
                for spin in range(2)
            ]
            for side in range(2)
        ]
        ahead = colour(2, received[0], False)
        behind = received[1]
        upper = subtracted(ahead, behind)
        lower = small_times(-singles[2][2:, :2], added(ahead, behind))
        rotate(g, upper + lower)

    def rotate(g, full):
        cols = group(g)
        for s in range(4):
            for c in range(3):
                real, imag = full[s][c]
                real = real + weave[0, s, c, cols, :]
                imag = imag + weave[1, s, c, cols, :]
                lanes_at = slice(c * plane, (c + 1) * plane)
                lanes_next = slice((3 + c) * plane, (4 + c) * plane)
                for number in range(moments):
                    cosine, sine = phases[number]
                    turned_real = (cosine * real + sine * imag).astype(jnp.bfloat16)
                    turned_imag = (cosine * imag - sine * real).astype(jnp.bfloat16)
                    at = number * width + 2 * s * GROUP
                    rows_at = slice(at, at + GROUP)
                    rows_next = slice(at + GROUP, at + 2 * GROUP)
                    weave_mm[g, rows_at, lanes_at] = turned_real
                    weave_mm[g, rows_at, lanes_next] = turned_imag
                    weave_mm[g, rows_next, lanes_at] = turned_imag
                    weave_mm[g, rows_next, lanes_next] = -turned_real

    def send_far(g, number):
        pl.when(here == 0)(chunk_copy(g, number, last, True).start)
        if g < groups - 1:
            pl.when(here == last)(chunk_copy(g, number, 1, True).start)
        else:
            pl.when((here == last) & (core == 1))(chunk_copy(g, number, 1, True).start)
            pl.when((here == last) & (core == 0))(far_copy(g, number).start)

    def send_first(g, number):
        if not relayed:
            for step in order:
                chunk_copy(g, number, step).start()
            return
        pl.when(inner)(chunk_copy(g, number, 1).start)
        pl.when(inner & jnp.logical_not(waiting))(chunk_copy(g, number, last).start)
        if g == groups - 1:
            pl.when(waiting)(chunk_copy(g, number, 2).start)

    def send_rest(those, phases_in=(0, 1)):
        for step in range(2, last):
            delayed = inner & (lax.rem(here + step, spaces) == far)
            for g in those:
                for number in range(moments):
                    if 0 in phases_in:
                        pl.when(jnp.logical_not(delayed))(chunk_copy(g, number, step).start)
        for step in (1, last):
            near = here == (0 if step == 1 else last)
            for g in those:
                for number in range(moments):
                    if 1 in phases_in:
                        pl.when(near)(chunk_copy(g, number, step).start)


    def product(g, rows_in):
        return lax.dot_general(
            rows_in, weave_mm[g], (((1,), (1,)), ((), ())), preferred_element_type=jnp.float32
        )

    far_owner = lax.div(far * rows, columns)
    far_row = pl.multiple_of(lax.rem(far * 4 * rows, 4 * columns), chunk_rows)
    def far_product(g):
        value = product(g, rows_scr[far_owner, pl.ds(far_row, chunk_rows), :])
        for number in range(moments):
            piece = value[:, number * width : (number + 1) * width]
            far_send[g, number] = piece.astype(jnp.bfloat16)
            send_far(g, number)

    def full_product(g):
        value = product(g, rows_scr[...].reshape(8 * columns, 6 * plane))
        for number in range(moments):
            for owner in range(spaces):
                piece = value[
                    owner * chunk_rows : (owner + 1) * chunk_rows,
                    number * width : (number + 1) * width,
                ]
                pair[g, number, owner] = piece
                chunk_send[g, number, owner] = piece.astype(jnp.bfloat16)
            send_first(g, number)

    for g in range(groups):
        depth_group(g)
        if relayed:
            pl.when(jnp.logical_not(inner))(functools.partial(far_product, g))
            pl.when(inner)(functools.partial(full_product, g))
        else:
            full_product(g)
    if relayed:

        @pl.when(jnp.logical_not(inner))
        def _():
            for g in range(groups):
                full_product(g)
                if g < groups - 1:
                    pl.when(core == 1)(functools.partial(send_rest, range(g, g + 1), (0,)))

    if relayed:
        @pl.when((core == 1) & jnp.logical_not(inner))
        def _():
            pl.semaphore_wait(ready_sem, 1)
            send_rest(range(groups - 1), (1,))
            send_rest(range(groups - 1, groups))

        @pl.when((core == 0) | inner)
        def _():
            send_rest(range(groups))

        @pl.when((core == 0) & (here == 0))
        def _():
            pl.semaphore_signal(ready_sem, inc=1, device_id={"spin": 1 - core})

    if relayed:
        for g in range(groups):
            for number in range(moments):
                for step in range(2, last):

                    @pl.when(((here == 1) & (step == last - 1)) | ((here == last - 1) & (step == 2) & ((core == 1) if g == groups - 1 else (core >= 0))))
                    def _(g=g, number=number, step=step):
                        chunk_copy(g, number, last, True).wait_recv()
                        target = lax.rem(here + step, spaces)
                        summed = pair[g, number, target] + relay_recv[g, number].astype(
                            jnp.float32
                        )
                        chunk_send[g, number, target] = summed.astype(jnp.bfloat16)
                        chunk_copy(g, number, step).start()

    def summed_piece(g, number):
        total = pair[g, number, here]
        for step in range(1, spaces):
            total = total + chunk_recv[number, g * last + step - 1].astype(jnp.float32)
        return total * scaling

    if relayed:

        @pl.when(waiting)
        def _():
            for g in range(groups):
                for number in range(moments):
                    chunk_copy(g, number, last).start()

    lane = lax.broadcasted_iota(jnp.int32, (rows, width), 1)
    slot = lax.div(lax.rem(lane, groups * GROUP), GROUP)
    back_copy.wait_send()
    wait_all(halo_send, halo_send_sem, halo_recv_sems.at[0]).wait_send()
    wait_all(chunk_send.at[:, :, :last], chunk_send_sem, chunk_recv_sems.at[0]).wait_send()
    if relayed:

        @pl.when((core == 0) & (here == last))
        def _():
            pl.semaphore_signal(ready_sem, inc=1, device_id={"spin": 1 - core})

    for number in range(moments):
        if number == 0:
            wait_chunks(0)
        elif number == 1:
            for other in range(1, moments):
                wait_chunks(other)
        totals = [summed_piece(g, number) for g in range(groups)]
        parts = []
        for part in range(2):
            merged_rows = []
            for s in range(4):
                merged = None
                for g in range(groups):
                    value = totals[g][s * rows : (s + 1) * rows]
                    if g != part:
                        value = pltpu.roll(value, (width + (g - part) * GROUP) % width, 1)
                    merged = value if merged is None else jnp.where(slot == g, value, merged)
                merged_rows.append(merged)
            parts.append(merged_rows)
        for offset in range(4):
            sums = []
            for part in range(2):
                terms = []
                for s in range(4):
                    t = s ^ offset
                    value = parts[part][s]
                    terms.append(pltpu.roll(value, width - t * 2 * GROUP, 1) if t else value)
                sums.append(
                    {
                        (pair_at, sign): terms[pair_at] + terms[pair_at + 1]
                        if sign > 0
                        else terms[pair_at] - terms[pair_at + 1]
                        for pair_at in (0, 2)
                        for sign in (1, -1)
                    }
                )
            for index in range(len(basis)):
                if np.flatnonzero(basis[index][0])[0] != offset:
                    continue
                units = [complex(basis[index][s, s ^ offset]) for s in range(4)]
                for part in range(2):
                    source, signs = picked(units, part)
                    first = sums[source][0, signs[0] * signs[1]]
                    second = sums[source][2, signs[2] * signs[3]]
                    results[number, index, part] = signed_sum(signs[0], first, signs[2], second)
        for k in range(gammas):
            for part in range(2):
                out_ref[part, number, k] = results[number, gamma_ref[k], part][:, :columns]


def store_kernel(value_ref, out_hbm, sems):
    moments = value_ref.shape[1]
    stores = [
        pltpu.make_async_copy(
            value_ref.at[:, number], out_hbm.at[:, number], sems.at[number]
        )
        for number in range(moments)
    ]
    for store in stores:
        store.start()
    for store in stores:
        store.wait()


def body(mesh, backward, forward, gauge_links, momenta, gamma_list):
    spaces = mesh.shape["space"]
    _, times, _, columns, _, layers, plane = forward.shape
    moments = momenta.shape[0]
    gammas = gamma_list.shape[0]
    rows = columns * mesh.shape["spin"] // spaces
    groups = columns // GROUP
    back = jnp.transpose(backward, (0, 1, 2, 4, 5, 3, 6)).reshape(2, 4, 3, columns, plane)
    fwd = jnp.transpose(forward, (0, 1, 2, 4, 5, 3, 6)).reshape(2, 4, 3, columns, plane)
    link = jnp.transpose(gauge_links, (1, 2, 3, 4, 5, 0, 6)).reshape(3, 3, 3, 2, plane)
    full_z = layers * spaces
    scaling = 0.5 / math.sqrt(3.0 * plane * full_z)
    width = 8 * GROUP
    vmem = pl.BlockSpec(memory_space=pltpu.VMEM)
    anywhere = pl.BlockSpec(memory_space=pl.ANY)
    out_shape = (2, moments, gammas, rows, columns)
    values = pl.pallas_call(
        functools.partial(kernel, spaces, LX, full_z, scaling),
        out_shape=pltpu.VMEM(out_shape, jnp.float32),
        in_specs=[anywhere] * 5,
        out_specs=vmem,
        scratch_shapes=[
            pltpu.VMEM(back.shape, back.dtype),
            pltpu.VMEM(fwd.shape, fwd.dtype),
            pltpu.VMEM(link.shape, link.dtype),
            pltpu.SMEM(momenta.shape, momenta.dtype),
            pltpu.SMEM(gamma_list.shape, gamma_list.dtype),
            pltpu.VMEM((2, 4, 3, columns, plane), jnp.bfloat16),
            pltpu.VMEM((moments, 16, 2, rows, width), jnp.float32),
            pltpu.VMEM((56, plane), jnp.float32),
            pltpu.VMEM((groups, 2, 2, 2, 3, GROUP, plane), jnp.bfloat16),
            pltpu.VMEM((groups, 2, 2, 2, 3, GROUP, plane), jnp.bfloat16),
            pltpu.VMEM((2, 4 * columns, 6 * plane), jnp.bfloat16),
            pltpu.VMEM((2, 4, 3, columns, plane), jnp.float32),
            pltpu.VMEM((groups, moments * width, 6 * plane), jnp.bfloat16),
            pltpu.VMEM((groups, moments, spaces, 4 * rows, width), jnp.float32),
            pltpu.VMEM((groups, moments, spaces, 4 * rows, width), jnp.bfloat16),
            pltpu.VMEM((groups, moments, 4 * rows, width), jnp.bfloat16),
            pltpu.VMEM((moments, groups * (spaces - 1), 4 * rows, width), jnp.bfloat16),
            pltpu.VMEM((groups, moments, 4 * rows, width), jnp.bfloat16),
            pltpu.SemaphoreType.DMA((5,)),
            pltpu.SemaphoreType.DMA((2,)),
            pltpu.SemaphoreType.DMA,
            pltpu.SemaphoreType.DMA((groups,)),
            pltpu.SemaphoreType.DMA,
            pltpu.SemaphoreType.DMA((moments,)),
            pltpu.SemaphoreType.DMA((groups, moments)),
            pltpu.SemaphoreType.REGULAR,
        ],
        compiler_params=pltpu.CompilerParams(collective_id=0, has_side_effects=True),
    )(back, fwd, link, momenta, gamma_list)
    out = pl.pallas_call(
        store_kernel,
        out_shape=jax.ShapeDtypeStruct(out_shape, jnp.float32),
        in_specs=[vmem],
        out_specs=anywhere,
        scratch_shapes=[pltpu.SemaphoreType.DMA((moments,))],
    )(pltpu.with_memory_space_constraint(values, pltpu.VMEM))
    return out.reshape(2, moments, gammas, times, rows, columns)


def solution(mesh):
    in_specs = (
        P("parts", "tm", None, "spin", None, "space", None),
        P("parts", "tm", None, "spin", None, "space", None),
        P("parts", None, None, None, "tm", "space", None),
        P(),
        P(),
    )
    out_specs = P("parts", None, None, "tm", "space", "spin")
    return jax.shard_map(
        functools.partial(body, mesh),
        mesh=mesh,
        in_specs=in_specs,
        out_specs=out_specs,
        check_vma=False,
    )
```
